128 devices in a mesh: gz: 128 (over y, z, x, core).
Axes of the slice: x: 4, y: 4, z: 4, core: 2. Of those that a mesh axis runs over, the one named last changes fastest.
Arguments:
- scores: int32 [512, 512, 512], P('gz'), may hold values from 0 to 134217727, as said below
Outputs:
- status: int32 [512, 512, 512], P('gz')
- counts: int32 [3], replicated
The draws below stay inside these ranges and needn't reach their ends.
Inputs may be any that keep to these rules, and one draw needn't show every extreme that they name: `scores`: all values distinct: a permutation of 0 to 134217727.
All inputs are finite; a program needn't handle non-finite values.
Results may differ from the reference program's by a relative error of at most 0.000001.
Values may be sent and summed in bfloat16 or wider, within the bound.
A program may use at most 64 MiB of HBM per device.

```python
import jax
import jax.numpy as jnp

NX = 512
NY = 512
ROUNDS = 3
NZ = 512


def draw_scores(key, part):
    return jax.random.permutation(key, NX * NY * NZ).astype(jnp.int32).reshape(NZ, NX, NY)


def setup_inputs(seed: int = 0) -> dict:
    splits = jax.random.split(jax.random.key(seed), 2)
    return {
        "scores": draw_scores(jax.random.fold_in(splits[1], 71), 0),
    }


ceiling = 1 << 30


def lateral_max(field):
    padded = jnp.pad(field, ((0, 0), (1, 1), (1, 1)))
    rows_max = jnp.maximum(jnp.maximum(padded[:, :-2, :], padded[:, 1:-1, :]), padded[:, 2:, :])
    return jnp.maximum(jnp.maximum(rows_max[:, :, :-2], rows_max[:, :, 1:-1]), rows_max[:, :, 2:])


def box_maximum(extended):
    depth_max = jnp.maximum(jnp.maximum(extended[:-2], extended[1:-1]), extended[2:])
    return lateral_max(depth_max)


def reference(scores):
    status = jnp.zeros(scores.shape, jnp.int32)
    totals = []
    for round_index in range(ROUNDS):
        labels = jnp.where(status == 0, 4 * scores + 4, jnp.where(status == 1, ceiling, 0)).astype(jnp.int32)
        near_max = box_maximum(jnp.pad(labels, ((1, 1), (0, 0), (0, 0))))
        far_max = box_maximum(jnp.pad(near_max, ((1, 1), (0, 0), (0, 0))))
        undecided = status == 0
        status = jnp.where(undecided & (far_max >= ceiling), 2,
                           jnp.where(undecided & (far_max == labels), 1, status)).astype(jnp.int32)
        totals.append(jnp.sum((status == 0).astype(jnp.int32)).astype(jnp.int32))
    return status, jnp.stack(totals).astype(jnp.int32)
```

```python
import functools

import jax
import jax.numpy as jnp
from jax import lax
from jax.experimental import pallas as pl
from jax.experimental.pallas import tpu as pltpu
from jax.sharding import PartitionSpec as P

DEPTH = 4
ROWS = 512
COLS = 512
LANES = 128
TILES = COLS // LANES
CHUNKS = 8
CHUNK = ROWS // CHUNKS
PAD = 8
ROOT = 1 << 28
MESH = pl.DeviceIdType.MESH


def cols(j):
    return slice(j * LANES, (j + 1) * LANES)


def lane_neighbours(tiles):
    shape = tiles[0].shape
    lane = lax.broadcasted_iota(jnp.int32, shape, 1)
    first, last = lane < 1, lane >= LANES - 1
    zero = jnp.zeros(shape, tiles[0].dtype)
    up = [pltpu.roll(t, 1, 1) for t in tiles]
    down = [pltpu.roll(t, LANES - 1, 1) for t in tiles]
    left = [jnp.where(first, up[j - 1] if j else zero, up[j]) for j in range(TILES)]
    right = [
        jnp.where(last, down[j + 1] if j < TILES - 1 else zero, down[j]) for j in range(TILES)
    ]
    return left, right


def lane_max5(tiles):
    left, right = lane_neighbours(tiles)
    three = [jnp.maximum(jnp.maximum(a, t), b) for a, t, b in zip(left, tiles, right)]
    left, right = lane_neighbours(three)
    return [jnp.maximum(a, b) for a, b in zip(left, right)]


def depth_max5(p):
    m34 = jnp.maximum(p[3], p[4])
    a = jnp.maximum(p[2], m34)
    a5 = jnp.maximum(a, p[5])
    return [
        jnp.maximum(jnp.maximum(p[0], p[1]), a),
        jnp.maximum(p[1], a5),
        jnp.maximum(a5, p[6]),
        jnp.maximum(jnp.maximum(m34, p[5]), jnp.maximum(p[6], p[7])),
    ]


def row_max5(t_ref, k, j, row, height):
    out = t_ref[k, j, pl.ds(row + PAD - 2, height), :]
    for d in (-1, 0, 1, 2):
        out = jnp.maximum(out, t_ref[k, j, pl.ds(row + PAD + d, height), :])
    return out


def kernel(
    n, x_ref, out_ref, count_ref,
    s_ref, l_ref, t1_ref, t2_ref, st_ref,
    send_lo1, send_hi1, recv_lo1, recv_hi1, send_lo2, send_hi2, recv_lo2, recv_hi2,
    load_sem, store_sem, send_sems, recv_sems,
):
    me = lax.axis_index("gz")
    right, left = lax.rem(me + 1, n), lax.rem(me + n - 1, n)
    keep_lo = jnp.where(me > 0, -1, 0).astype(jnp.int32)
    keep_hi = jnp.where(me < n - 1, -1, 0).astype(jnp.int32)
    live_lo = jnp.where(me > 0, 0.0, 100.0).astype(jnp.float32)
    live_hi = jnp.where(me < n - 1, 0.0, 100.0).astype(jnp.float32)

    def rows_of(c):
        return pl.ds(pl.multiple_of(c * CHUNK, CHUNK), CHUNK)

    def load(c):
        return pltpu.make_async_copy(
            x_ref.at[:, rows_of(c), :], s_ref.at[pl.ds(2, DEPTH), rows_of(c), :], load_sem.at[c]
        )

    def store(c):
        return pltpu.make_async_copy(
            st_ref.at[:, rows_of(c), :], out_ref.at[:, rows_of(c), :], store_sem.at[c]
        )

    def remote(src, dst, stage, side, c, device):
        return pltpu.make_async_remote_copy(
            src_ref=src, dst_ref=dst,
            send_sem=send_sems.at[stage, side, c], recv_sem=recv_sems.at[stage, side, c],
            device_id=(device,), device_id_type=MESH,
        )

    def planes(c):
        r = rows_of(c)
        return (
            remote(s_ref.at[pl.ds(2, 2), r, :], s_ref.at[pl.ds(6, 2), r, :], 0, 1, c, left),
            remote(s_ref.at[pl.ds(4, 2), r, :], s_ref.at[pl.ds(0, 2), r, :], 0, 0, c, right),
        )

    def roots1(c):
        r = rows_of(c)
        return (
            remote(send_lo1.at[r, :], recv_hi1.at[r, :], 1, 1, c, left),
            remote(send_hi1.at[r, :], recv_lo1.at[r, :], 1, 0, c, right),
        )

    def roots2(c):
        r = rows_of(c)
        return (
            remote(send_lo2.at[r, :], recv_hi2.at[r, :], 2, 1, c, left),
            remote(send_hi2.at[r, :], recv_lo2.at[r, :], 2, 0, c, right),
        )

    def start(pair):
        for copy in pair:
            copy.start()

    def wait_recv(pair):
        for copy in pair:
            copy.wait_recv()

    def wait_send(pair):
        for copy in pair:
            copy.wait_send()

    def loop(count, body):
        def step(i, carry):
            body(i)
            return carry
        lax.fori_loop(0, count, step, 0)

    loop(CHUNKS, lambda c: load(c).start())
    barrier = pltpu.get_barrier_semaphore()
    for neighbour in (left, right):
        pl.semaphore_signal(barrier, inc=1, device_id=(neighbour,), device_id_type=MESH)
    for ref, depth in ((t1_ref, 4), (t2_ref, 8)):
        for k in range(depth):
            for j in range(TILES):
                ref[k, j, 0:PAD, :] = jnp.zeros((PAD, LANES), jnp.int32)
                ref[k, j, PAD + ROWS:, :] = jnp.zeros((PAD, LANES), jnp.int32)
    for k in range(3):
        count_ref[k] = jnp.zeros((8, LANES), jnp.int32)
    pl.semaphore_wait(barrier, 2)

    def send_planes(c):
        load(c).wait()
        start(planes(c))

    loop(CHUNKS, send_planes)

    def rounds(first, second, arrive, leave):
        def step(c):
            @pl.when(c < CHUNKS)
            def _():
                arrive(c)
                first(c)

            @pl.when(c > 0)
            def _():
                second(c - 1)
                leave(c - 1)
        loop(CHUNKS + 1, step)

    def over_rows(c, height, body):
        loop(CHUNK // height, lambda i: body(pl.multiple_of(c * CHUNK + i * height, height)))

    def add_count(k, flags):
        total = flags[0]
        for f in flags[1:]:
            total = total + f
        count_ref[k] += total[:8] + total[8:]

    def first1(c):
        def body(row):
            outs = []
            for j in range(TILES):
                p = [s_ref[k, pl.ds(row, 8), cols(j)] for k in range(8)]
                p[0], p[1] = p[0] & keep_lo, p[1] & keep_lo
                p[6], p[7] = p[6] & keep_hi, p[7] & keep_hi
                outs.append(depth_max5(p))
            for k in range(DEPTH):
                for j, t in enumerate(lane_max5([o[k] for o in outs])):
                    t1_ref[k, j, pl.ds(row + PAD, 8), :] = t
        over_rows(c, 8, body)

    def second1(c):
        def body(row):
            flags = []
            for j in range(TILES):
                roots = []
                for k in range(DEPTH):
                    s = s_ref[2 + k, pl.ds(row, 16), cols(j)]
                    root = row_max5(t1_ref, k, j, row, 16) == s
                    l_ref[2 + k, pl.ds(row, 16), cols(j)] = jnp.where(root, ROOT, s)
                    flags.append(jnp.where(root, 0, 1))
                    roots.append(root)
                lo = jnp.zeros((16, LANES), jnp.float32)
                hi = lo
                for k in range(DEPTH):
                    hi = jnp.where(roots[k], float(DEPTH - k), hi)
                    lo = jnp.where(roots[DEPTH - 1 - k], float(DEPTH - k), lo)
                send_lo1[pl.ds(row, 16), cols(j)] = lo.astype(jnp.bfloat16)
                send_hi1[pl.ds(row, 16), cols(j)] = hi.astype(jnp.bfloat16)
            add_count(0, flags)
        over_rows(c, 16, body)

    rounds(first1, second1, lambda c: wait_recv(planes(c)), lambda c: start(roots1(c)))

    def first2(c):
        def body(row):
            for j in range(TILES):
                at = (pl.ds(row, 16), cols(j))
                d_lo = recv_lo1[at].astype(jnp.float32) + live_lo
                d_hi = recv_hi1[at].astype(jnp.float32) + live_hi
                far = [
                    jnp.where(d_lo == 4.0, ROOT, 0), jnp.where(d_lo == 3.0, ROOT, 0),
                    jnp.where(d_hi == 3.0, ROOT, 0), jnp.where(d_hi == 4.0, ROOT, 0),
                ]
                p = [
                    jnp.where(d_lo == 2.0, ROOT, s_ref[(0,) + at] & keep_lo),
                    jnp.where(d_lo == 1.0, ROOT, s_ref[(1,) + at] & keep_lo),
                    *(l_ref[(k,) + at] for k in range(2, 6)),
                    jnp.where(d_hi == 1.0, ROOT, s_ref[(6,) + at] & keep_hi),
                    jnp.where(d_hi == 2.0, ROOT, s_ref[(7,) + at] & keep_hi),
                ]
                for k in (0, 1, 6, 7):
                    l_ref[(k,) + at] = p[k]
                mine = depth_max5(p)
                low = jnp.maximum(jnp.maximum(far[1], p[0]), jnp.maximum(p[1], p[2]))
                high = jnp.maximum(jnp.maximum(far[2], p[7]), jnp.maximum(p[6], p[5]))
                outs = [
                    jnp.maximum(low, far[0]), jnp.maximum(low, p[3]), *mine,
                    jnp.maximum(high, p[4]), jnp.maximum(high, far[3]),
                ]
                for k in range(8):
                    t2_ref[k, j, pl.ds(row + PAD, 16), :] = outs[k]
            for k in range(8):
                tiles = [t2_ref[k, j, pl.ds(row + PAD, 16), :] for j in range(TILES)]
                for j, t in enumerate(lane_max5(tiles)):
                    t2_ref[k, j, pl.ds(row + PAD, 16), :] = t
        over_rows(c, 16, body)

    def second2(c):
        def body(row):
            flags = []
            for j in range(TILES):
                at = (pl.ds(row, 16), cols(j))
                roots = []
                for k in range(DEPTH):
                    l = l_ref[(2 + k,) + at]
                    top = row_max5(t2_ref, 2 + k, j, row, 16)
                    root, near = top == l, top >= ROOT
                    l_ref[(2 + k,) + at] = jnp.where(root, ROOT, jnp.where(near, 0, l))
                    flags.append(jnp.where(root | near, 0, 1))
                    roots.append(root)
                for k in (0, 1, 6, 7):
                    l = l_ref[(k,) + at]
                    top = row_max5(t2_ref, k, j, row, 16)
                    l_ref[(k,) + at] = jnp.where(top >= ROOT, l & ROOT, l)
                lo = jnp.where(roots[0], 1.0, jnp.where(roots[1], 2.0, 0.0))
                hi = jnp.where(roots[3], 1.0, jnp.where(roots[2], 2.0, 0.0))
                send_lo2[at] = lo.astype(jnp.bfloat16)
                send_hi2[at] = hi.astype(jnp.bfloat16)
            add_count(1, flags)
        over_rows(c, 16, body)

    rounds(first2, second2, lambda c: wait_recv(roots1(c)), lambda c: start(roots2(c)))

    def first3(c):
        def body(row):
            for j in range(TILES):
                at = (pl.ds(row, 16), cols(j))
                d_lo = recv_lo2[at].astype(jnp.float32) + live_lo
                d_hi = recv_hi2[at].astype(jnp.float32) + live_hi
                p = [l_ref[(k,) + at] for k in range(8)]
                p[0] = jnp.where(d_lo == 2.0, ROOT, p[0])
                p[1] = jnp.where(d_lo == 1.0, ROOT, p[1])
                p[6] = jnp.where(d_hi == 1.0, ROOT, p[6])
                p[7] = jnp.where(d_hi == 2.0, ROOT, p[7])
                for k, t in enumerate(depth_max5(p)):
                    t1_ref[k, j, pl.ds(row + PAD, 16), :] = t
            for k in range(DEPTH):
                tiles = [t1_ref[k, j, pl.ds(row + PAD, 16), :] for j in range(TILES)]
                for j, t in enumerate(lane_max5(tiles)):
                    t1_ref[k, j, pl.ds(row + PAD, 16), :] = t
        over_rows(c, 16, body)

    def second3(c):
        def body(row):
            flags = []
            for j in range(TILES):
                at = (pl.ds(row, 16), cols(j))
                for k in range(DEPTH):
                    l = l_ref[(2 + k,) + at]
                    top = row_max5(t1_ref, k, j, row, 16)
                    root, near = top == l, top >= ROOT
                    st_ref[(k,) + at] = jnp.where(root, 1, jnp.where(near, 2, 0))
                    flags.append(jnp.where(root | near, 0, 1))
            add_count(2, flags)
        over_rows(c, 16, body)

    rounds(first3, second3, lambda c: wait_recv(roots2(c)), lambda c: store(c).start())

    def drain(c):
        wait_send(planes(c))
        wait_send(roots1(c))
        wait_send(roots2(c))
        store(c).wait()

    loop(CHUNKS, drain)


def shards(n, scores):
    field = pltpu.VMEM((2 * DEPTH, ROWS, COLS), jnp.int32)
    column = pltpu.VMEM((ROWS, COLS), jnp.bfloat16)

    def wide(depth):
        return pltpu.VMEM((depth, TILES, ROWS + 2 * PAD, LANES), jnp.int32)

    status, counts = pl.pallas_call(
        functools.partial(kernel, n),
        out_shape=(
            jax.ShapeDtypeStruct((DEPTH, ROWS, COLS), jnp.int32),
            jax.ShapeDtypeStruct((3, 8, LANES), jnp.int32),
        ),
        in_specs=[pl.BlockSpec(memory_space=pl.ANY)],
        out_specs=(
            pl.BlockSpec(memory_space=pl.ANY),
            pl.BlockSpec(memory_space=pltpu.VMEM),
        ),
        scratch_shapes=[
            field, field, wide(DEPTH), wide(2 * DEPTH),
            pltpu.VMEM((DEPTH, ROWS, COLS), jnp.int32),
            *[column] * 8,
            pltpu.SemaphoreType.DMA((CHUNKS,)),
            pltpu.SemaphoreType.DMA((CHUNKS,)),
            pltpu.SemaphoreType.DMA((3, 2, CHUNKS)),
            pltpu.SemaphoreType.DMA((3, 2, CHUNKS)),
        ],
        compiler_params=pltpu.CompilerParams(
            collective_id=0, has_side_effects=True, vmem_limit_bytes=56 << 20
        ),
    )(scores)
    return status, lax.psum(jnp.sum(counts, axis=(1, 2)), "gz")


def solution(mesh):
    n = mesh.shape["gz"]
    return jax.shard_map(
        functools.partial(shards, n),
        mesh=mesh,
        in_specs=(P("gz", None, None),),
        out_specs=(P("gz", None, None), P()),
        check_vma=False,
    )
```

```python
import functools

import jax
import jax.numpy as jnp
from jax import lax
from jax.experimental import pallas as pl
from jax.experimental.pallas import tpu as pltpu
from jax.sharding import PartitionSpec as P

DEPTH = 4
ROWS = 512
COLS = 512
LANES = 128
TILES = COLS // LANES
CHUNK = 32
CHUNKS = ROWS // CHUNK
STEP = 16
PAD = 8
GROUPS = (8, 4, 4)
ROOT = float(1 << 40)
MANTISSA = 23
MESH = pl.DeviceIdType.MESH


def cols(j):
    return slice(j * LANES, (j + 1) * LANES)


def shifted(tiles, by):
    shape = tiles[0].shape
    lane = lax.broadcasted_iota(jnp.int32, shape, 1)
    zero = jnp.zeros(shape, tiles[0].dtype)
    moved = [pltpu.roll(t, by % LANES, 1) for t in tiles]
    if by > 0:
        return [jnp.where(lane < by, moved[j - 1] if j else zero, moved[j]) for j in range(TILES)]
    return [
        jnp.where(lane >= LANES + by, moved[j + 1] if j < TILES - 1 else zero, moved[j])
        for j in range(TILES)
    ]


def lane_window(tiles, join):
    sides = [shifted(tiles, by) for by in (1, -1, 2, -2)]
    return [
        join(join(join(a, b), join(c, d)), t) for a, b, c, d, t in zip(*sides, tiles)
    ]


def depth_max5(p):
    m34 = jnp.maximum(p[3], p[4])
    a = jnp.maximum(p[2], m34)
    a5 = jnp.maximum(a, p[5])
    return [
        jnp.maximum(jnp.maximum(p[0], p[1]), a),
        jnp.maximum(p[1], a5),
        jnp.maximum(a5, p[6]),
        jnp.maximum(jnp.maximum(m34, p[5]), jnp.maximum(p[6], p[7])),
    ]


def row_window(ref, at, row, join):
    parts = [ref[(*at, pl.ds(row + PAD + d, STEP), slice(None))] for d in (-2, -1, 0, 1, 2)]
    return join(join(join(parts[0], parts[1]), join(parts[3], parts[4])), parts[2])


def embed(s):
    low = (s & ((1 << MANTISSA) - 1)) | (1 << MANTISSA)
    high = jnp.left_shift(jnp.ones_like(s), jnp.right_shift(s, MANTISSA))
    return low.astype(jnp.float32) * high.astype(jnp.float32)


def kernel(
    n, x_ref, out_ref, count_ref,
    x_buf, f_ref, l1_ref, l2_ref, gone_ref, t_ref, g_ref, st_ref,
    send_lo1, send_hi1, recv_lo1, recv_hi1, send_lo2, send_hi2, recv_lo2, recv_hi2,
    tally, part, parts,
    load_sem, store_sem, send_sems, recv_sems, part_send, part_recv,
):
    me = lax.axis_index("gz")
    right, left = lax.rem(me + 1, n), lax.rem(me + n - 1, n)
    keep_lo = jnp.where(me > 0, 1.0, 0.0).astype(jnp.float32)
    keep_hi = jnp.where(me < n - 1, 1.0, 0.0).astype(jnp.float32)

    partners = []
    stride = 1
    for size in GROUPS:
        place = lax.rem(lax.div(me, stride), size)
        partners.append(
            [me + (lax.rem(place + o, size) - place) * stride for o in range(1, size)]
        )
        stride *= size

    def rows_of(c):
        return pl.ds(pl.multiple_of(c * CHUNK, CHUNK), CHUNK)

    def load(c):
        return pltpu.make_async_copy(
            x_ref.at[:, rows_of(c), :], x_buf.at[:, rows_of(c), :], load_sem.at[c]
        )

    def store(c):
        return pltpu.make_async_copy(
            st_ref.at[:, rows_of(c), :], out_ref.at[:, rows_of(c), :], store_sem.at[c]
        )

    def remote(src, dst, stage, side, c, device):
        return pltpu.make_async_remote_copy(
            src_ref=src, dst_ref=dst,
            send_sem=send_sems.at[stage, side, c], recv_sem=recv_sems.at[stage, side, c],
            device_id=(device,), device_id_type=MESH,
        )

    def planes(c):
        r = rows_of(c)
        return (
            remote(f_ref.at[pl.ds(2, 2), r, :], f_ref.at[pl.ds(6, 2), r, :], 0, 1, c, left),
            remote(f_ref.at[pl.ds(4, 2), r, :], f_ref.at[pl.ds(0, 2), r, :], 0, 0, c, right),
        )

    def roots1(c):
        r = rows_of(c)
        return (
            remote(send_lo1.at[r, :], recv_hi1.at[r, :], 1, 1, c, left),
            remote(send_hi1.at[r, :], recv_lo1.at[r, :], 1, 0, c, right),
        )

    def roots2(c):
        r = rows_of(c)
        return (
            remote(send_lo2.at[r, :], recv_hi2.at[r, :], 2, 1, c, left),
            remote(send_hi2.at[r, :], recv_lo2.at[r, :], 2, 0, c, right),
        )

    def start(pair):
        for copy in pair:
            copy.start()

    def wait_recv(pair):
        for copy in pair:
            copy.wait_recv()

    def wait_send(pair):
        for copy in pair:
            copy.wait_send()

    def loop(first, last, body):
        def step(i, carry):
            body(i)
            return carry
        lax.fori_loop(first, last, step, 0)

    def over_rows(c, body):
        loop(0, CHUNK // STEP, lambda i: body(pl.multiple_of(c * CHUNK + i * STEP, STEP)))

    loop(0, CHUNKS, lambda c: load(c).start())
    barrier = pltpu.get_barrier_semaphore()
    greeted = [left, right, *(p for group in partners for p in group)]
    for other in greeted:
        pl.semaphore_signal(barrier, inc=1, device_id=(other,), device_id_type=MESH)
    for j in range(TILES):
        for edge in (slice(0, PAD), slice(PAD + ROWS, 2 * PAD + ROWS)):
            for k in range(DEPTH):
                t_ref[k, j, edge, :] = jnp.zeros((PAD, LANES), jnp.float32)
            g_ref[j, edge, :] = jnp.zeros((PAD, LANES), jnp.int32)
    for k in range(3):
        tally[k] = jnp.zeros((8, LANES), jnp.int32)

    def prepare(c):
        load(c).wait()

        def body(row):
            for k in range(DEPTH):
                for j in range(TILES):
                    at = (pl.ds(row, STEP), cols(j))
                    f_ref[(2 + k,) + at] = embed(x_buf[(k,) + at])
        over_rows(c, body)

    def send_planes(c):
        prepare(c)
        start(planes(c))

    prepare(0)
    pl.semaphore_wait(barrier, len(greeted))
    start(planes(0))
    loop(1, CHUNKS, send_planes)

    def rounds(first, second, arrive, leave):
        arrive(0)
        over_rows(0, first)

        def step(c):
            arrive(c)

            def body(row):
                second(pl.multiple_of(row - CHUNK, STEP))
                first(row)
            over_rows(c, body)
            leave(c - 1)
        loop(1, CHUNKS, step)
        over_rows(CHUNKS - 1, second)
        leave(CHUNKS - 1)

    def add_count(k, flags):
        while len(flags) > 1:
            flags = [a + b for a, b in zip(flags[::2], flags[1::2])]
        tally[k] += flags[0][:8] + flags[0][8:]

    def laterals(outs):
        for k in range(DEPTH):
            yield k, lane_window([o[k] for o in outs], jnp.maximum)

    def put(row, outs):
        for k, tiles in laterals(outs):
            for j, t in enumerate(tiles):
                t_ref[k, j, pl.ds(row + PAD, STEP), :] = t

    def first1(row):
        outs = []
        for j in range(TILES):
            at = (pl.ds(row, STEP), cols(j))
            p = [f_ref[(k,) + at] for k in range(8)]
            for k, keep in ((0, keep_lo), (1, keep_lo), (6, keep_hi), (7, keep_hi)):
                p[k] = p[k] * keep
                f_ref[(k,) + at] = p[k]
            outs.append(depth_max5(p))
        put(row, outs)

    def second1(row):
        flags = []
        for j in range(TILES):
            at = (pl.ds(row, STEP), cols(j))
            roots = []
            for k in range(DEPTH):
                s = f_ref[(2 + k,) + at]
                root = row_window(t_ref, (k, j), row, jnp.maximum) == s
                l1_ref[(k,) + at] = jnp.where(root, ROOT, s)
                flags.append(jnp.where(root, 0, 1))
                roots.append(root)
            lo = jnp.zeros((STEP, LANES), jnp.float32)
            hi = lo
            for k in range(DEPTH):
                hi = jnp.where(roots[k], float(DEPTH - k), hi)
                lo = jnp.where(roots[DEPTH - 1 - k], float(DEPTH - k), lo)
            send_lo1[at] = lo.astype(jnp.bfloat16)
            send_hi1[at] = hi.astype(jnp.bfloat16)
        add_count(0, flags)

    rounds(first1, second1, lambda c: wait_recv(planes(c)), lambda c: start(roots1(c)))

    def first2(row):
        outs, marks = [], []
        for j in range(TILES):
            at = (pl.ds(row, STEP), cols(j))
            d_lo = recv_lo1[at].astype(jnp.float32) * keep_lo
            d_hi = recv_hi1[at].astype(jnp.float32) * keep_hi
            mine = [l1_ref[(k,) + at] for k in range(DEPTH)]
            outs.append(depth_max5([
                jnp.where(d_lo == 2.0, ROOT, f_ref[(0,) + at]),
                jnp.where(d_lo == 1.0, ROOT, f_ref[(1,) + at]),
                *mine,
                jnp.where(d_hi == 1.0, ROOT, f_ref[(6,) + at]),
                jnp.where(d_hi == 2.0, ROOT, f_ref[(7,) + at]),
            ]))
            mark = jnp.where(d_lo > 3.5, 1, jnp.where(d_lo > 0.5, 3, 0))
            mark |= jnp.where(d_hi > 3.5, 8, jnp.where(d_hi > 0.5, 12, 0))
            for value, bits in zip(mine, (3, 2, 4, 12)):
                mark |= jnp.where(value == ROOT, bits, 0)
            marks.append(mark)
        put(row, outs)
        for j, t in enumerate(lane_window(marks, jnp.bitwise_or)):
            g_ref[j, pl.ds(row + PAD, STEP), :] = t

    def second2(row):
        flags = []
        for j in range(TILES):
            at = (pl.ds(row, STEP), cols(j))
            roots = []
            for k in range(DEPTH):
                l = l1_ref[(k,) + at]
                top = row_window(t_ref, (k, j), row, jnp.maximum)
                root, near = top == l, top >= ROOT
                value = jnp.where(root, ROOT, jnp.where(near, 0.0, l))
                l2_ref[(k,) + at] = value
                flags.append(jnp.where(root | near, 0, 1))
                roots.append(root)
            gone_ref[at] = row_window(g_ref, (j,), row, jnp.bitwise_or)
            lo = jnp.where(roots[0], 1.0, jnp.where(roots[1], 2.0, 0.0))
            hi = jnp.where(roots[3], 1.0, jnp.where(roots[2], 2.0, 0.0))
            send_lo2[at] = lo.astype(jnp.bfloat16)
            send_hi2[at] = hi.astype(jnp.bfloat16)
        add_count(1, flags)

    rounds(first2, second2, lambda c: wait_recv(roots1(c)), lambda c: start(roots2(c)))

    def first3(row):
        outs = []
        for j in range(TILES):
            at = (pl.ds(row, STEP), cols(j))
            d_lo = recv_lo2[at].astype(jnp.float32) * keep_lo
            d_hi = recv_hi2[at].astype(jnp.float32) * keep_hi
            gone = gone_ref[at]

            def halo(k, bit, is_root):
                left_over = jnp.where((gone & bit) == 0, f_ref[(k,) + at], 0.0)
                return jnp.where(is_root, ROOT, left_over)

            outs.append(depth_max5([
                halo(0, 1, d_lo == 2.0), halo(1, 2, d_lo == 1.0),
                *(l2_ref[(k,) + at] for k in range(DEPTH)),
                halo(6, 4, d_hi == 1.0), halo(7, 8, d_hi == 2.0),
            ]))
        put(row, outs)

    def second3(row):
        flags = []
        for j in range(TILES):
            at = (pl.ds(row, STEP), cols(j))
            for k in range(DEPTH):
                top = row_window(t_ref, (k, j), row, jnp.maximum)
                root, near = top == l2_ref[(k,) + at], top >= ROOT
                state = jnp.where(root, 1.0, jnp.where(near, 2.0, 0.0))
                st_ref[(k,) + at] = state.astype(jnp.bfloat16)
                flags.append(jnp.where(root | near, 0, 1))
        add_count(2, flags)

    rounds(first3, second3, lambda c: wait_recv(roots2(c)), lambda c: store(c).start())

    for k in range(3):
        part[0, k:k + 1, :] = jnp.sum(tally[k], axis=0, keepdims=True)
    part[0, 3:8, :] = jnp.zeros((5, LANES), jnp.int32)
    slot = 0
    for stage, group in enumerate(partners):
        copies = [
            pltpu.make_async_remote_copy(
                src_ref=part.at[stage], dst_ref=parts.at[slot + o],
                send_sem=part_send.at[slot + o], recv_sem=part_recv.at[slot + o],
                device_id=(other,), device_id_type=MESH,
            )
            for o, other in enumerate(group)
        ]
        start(copies)
        total = part[stage]
        for o, copy in enumerate(copies):
            copy.wait_recv()
            total = total + parts[slot + o]
        part[stage + 1] = total
        wait_send(copies)
        slot += len(group)
    for k in range(3):
        count_ref[k] = jnp.sum(part[len(GROUPS), k:k + 1, :])

    def drain(c):
        wait_send(planes(c))
        wait_send(roots1(c))
        wait_send(roots2(c))
        store(c).wait()

    loop(0, CHUNKS, drain)


def shards(n, scores):
    slab = (DEPTH, ROWS, COLS)
    column = pltpu.VMEM((ROWS, COLS), jnp.bfloat16)
    slots = sum(GROUPS) - len(GROUPS)
    status, counts = pl.pallas_call(
        functools.partial(kernel, n),
        out_shape=(
            jax.ShapeDtypeStruct(slab, jnp.bfloat16),
            jax.ShapeDtypeStruct((3,), jnp.int32),
        ),
        in_specs=[pl.BlockSpec(memory_space=pl.ANY)],
        out_specs=(
            pl.BlockSpec(memory_space=pl.ANY),
            pl.BlockSpec(memory_space=pltpu.SMEM),
        ),
        scratch_shapes=[
            pltpu.VMEM(slab, jnp.int32),
            pltpu.VMEM((2 * DEPTH, ROWS, COLS), jnp.float32),
            pltpu.VMEM(slab, jnp.float32),
            pltpu.VMEM(slab, jnp.float32),
            pltpu.VMEM((ROWS, COLS), jnp.int32),
            pltpu.VMEM((DEPTH, TILES, ROWS + 2 * PAD, LANES), jnp.float32),
            pltpu.VMEM((TILES, ROWS + 2 * PAD, LANES), jnp.int32),
            pltpu.VMEM(slab, jnp.bfloat16),
            *[column] * 8,
            pltpu.VMEM((3, 8, LANES), jnp.int32),
            pltpu.VMEM((len(GROUPS) + 1, 8, LANES), jnp.int32),
            pltpu.VMEM((slots, 8, LANES), jnp.int32),
            pltpu.SemaphoreType.DMA((CHUNKS,)),
            pltpu.SemaphoreType.DMA((CHUNKS,)),
            pltpu.SemaphoreType.DMA((3, 2, CHUNKS)),
            pltpu.SemaphoreType.DMA((3, 2, CHUNKS)),
            pltpu.SemaphoreType.DMA((slots,)),
            pltpu.SemaphoreType.DMA((slots,)),
        ],
        compiler_params=pltpu.CompilerParams(
            collective_id=0, has_side_effects=True, vmem_limit_bytes=56 << 20
        ),
    )(scores)
    return status.astype(jnp.int32), counts


def solution(mesh):
    n = mesh.shape["gz"]
    return jax.shard_map(
        functools.partial(shards, n),
        mesh=mesh,
        in_specs=(P("gz", None, None),),
        out_specs=(P("gz", None, None), P()),
        check_vma=False,
    )
```

```python
import functools

import jax
import jax.numpy as jnp
from jax import lax
from jax.experimental import pallas as pl
from jax.experimental.pallas import tpu as pltpu
from jax.sharding import PartitionSpec as P

DEPTH = 4
ROWS = 512
COLS = 512
LANES = 128
TILES = 4
BLOCK = LANES // TILES
CHUNK = 32
CHUNKS = ROWS // CHUNK
STEP = 16
PAD = 8
GROUPS = (8, 4, 4)
ROOT = float(1 << 40)
MANTISSA = 23
MESH = pl.DeviceIdType.MESH


def cols(j):
    return slice(j * LANES, (j + 1) * LANES)


def gather(x, index):
    halves = [
        jnp.take_along_axis(x[r:r + 8], index, axis=1, mode="promise_in_bounds")
        for r in range(0, x.shape[0], 8)
    ]
    return jnp.concatenate(halves, axis=0)


def lane_of(height):
    return lax.broadcasted_iota(jnp.int32, (height, LANES), 1)


def by_block(tiles, source):
    block = lane_of(tiles[0].shape[0]) // BLOCK
    out = []
    for a in range(TILES):
        t = tiles[source(TILES - 1, a)]
        for p in range(TILES - 1):
            t = jnp.where(block == p, tiles[source(p, a)], t)
        out.append(t)
    return out


def interleave(tiles):
    lane = lane_of(8)
    sorted_ = [
        gather(t, (lane % BLOCK) * TILES + (lane // BLOCK + TILES - s) % TILES)
        for s, t in enumerate(tiles)
    ]
    mixed = by_block(sorted_, lambda p, j: (p - j) % TILES)
    return [pltpu.roll(t, LANES - BLOCK * j, 1) if j else t for j, t in enumerate(mixed)]


def natural(tiles):
    lane = lane_of(8)
    turned = [pltpu.roll(t, BLOCK * j, 1) if j else t for j, t in enumerate(tiles)]
    mixed = by_block(turned, lambda p, s: (p - s) % TILES)
    return [
        gather(t, BLOCK * ((lane % TILES + s) % TILES) + lane // TILES)
        for s, t in enumerate(mixed)
    ]


def column_sides(t):
    lane = lane_of(t[0].shape[0])
    zero = jnp.zeros(t[0].shape, t[0].dtype)
    before = [jnp.where(lane == 0, zero, pltpu.roll(t[j], 1, 1)) for j in (2, 3)]
    after = [jnp.where(lane == LANES - 1, zero, pltpu.roll(t[j], LANES - 1, 1)) for j in (0, 1)]
    return (*before, *after)


def column_window(t, sides, join):
    r2, r3, l0, l1 = sides
    m12 = join(t[1], t[2])
    m012, m123 = join(t[0], m12), join(m12, t[3])
    whole = join(m012, t[3])
    return [join(m012, join(r2, r3)), join(whole, r3), join(whole, l0), join(m123, join(l0, l1))]


def depth_max5(p):
    m34 = jnp.maximum(p[3], p[4])
    a = jnp.maximum(p[2], m34)
    a5 = jnp.maximum(a, p[5])
    return [
        jnp.maximum(jnp.maximum(p[0], p[1]), a),
        jnp.maximum(p[1], a5),
        jnp.maximum(a5, p[6]),
        jnp.maximum(jnp.maximum(m34, p[5]), jnp.maximum(p[6], p[7])),
    ]


def row_window(ref, at, row, join):
    parts = [ref[(*at, pl.ds(row + PAD + d, STEP), slice(None))] for d in (-2, -1, 0, 1, 2)]
    return join(join(join(parts[0], parts[1]), join(parts[3], parts[4])), parts[2])


def embed(s):
    low = (s & ((1 << MANTISSA) - 1)) | (1 << MANTISSA)
    high = jnp.left_shift(jnp.ones_like(s), jnp.right_shift(s, MANTISSA))
    return low.astype(jnp.float32) * high.astype(jnp.float32)


def kernel(
    n, x_ref, out_ref, count_ref,
    x_buf, f_ref, l1_ref, l2_ref, gone_ref, t_ref, g_ref, st_ref,
    send_lo1, send_hi1, recv_lo1, recv_hi1, send_lo2, send_hi2, recv_lo2, recv_hi2,
    tally, part, parts,
    load_sem, store_sem, send_sems, recv_sems, part_send, part_recv,
):
    me = lax.axis_index("gz")
    right, left = lax.rem(me + 1, n), lax.rem(me + n - 1, n)
    keep_lo = jnp.where(me > 0, 1.0, 0.0).astype(jnp.float32)
    keep_hi = jnp.where(me < n - 1, 1.0, 0.0).astype(jnp.float32)

    partners = []
    stride = 1
    for size in GROUPS:
        place = lax.rem(lax.div(me, stride), size)
        partners.append(
            [me + (lax.rem(place + o, size) - place) * stride for o in range(1, size)]
        )
        stride *= size

    def rows_of(c):
        return pl.ds(pl.multiple_of(c * CHUNK, CHUNK), CHUNK)

    def load(c):
        return pltpu.make_async_copy(
            x_ref.at[:, rows_of(c), :], x_buf.at[:, rows_of(c), :], load_sem.at[c]
        )

    def store(c):
        return pltpu.make_async_copy(
            st_ref.at[rows_of(c), :], out_ref.at[rows_of(c), :], store_sem.at[c]
        )

    def remote(src, dst, stage, side, c, device):
        return pltpu.make_async_remote_copy(
            src_ref=src, dst_ref=dst,
            send_sem=send_sems.at[stage, side, c], recv_sem=recv_sems.at[stage, side, c],
            device_id=(device,), device_id_type=MESH,
        )

    def planes(c):
        r = rows_of(c)
        return (
            remote(f_ref.at[pl.ds(2, 2), r, :], f_ref.at[pl.ds(6, 2), r, :], 0, 1, c, left),
            remote(f_ref.at[pl.ds(4, 2), r, :], f_ref.at[pl.ds(0, 2), r, :], 0, 0, c, right),
        )

    def roots1(c):
        r = rows_of(c)
        return (
            remote(send_lo1.at[r, :], recv_hi1.at[r, :], 1, 1, c, left),
            remote(send_hi1.at[r, :], recv_lo1.at[r, :], 1, 0, c, right),
        )

    def roots2(c):
        r = rows_of(c)
        return (
            remote(send_lo2.at[r, :], recv_hi2.at[r, :], 2, 1, c, left),
            remote(send_hi2.at[r, :], recv_lo2.at[r, :], 2, 0, c, right),
        )

    def start(pair):
        for copy in pair:
            copy.start()

    def wait_recv(pair):
        for copy in pair:
            copy.wait_recv()

    def wait_send(pair):
        for copy in pair:
            copy.wait_send()

    def loop(first, last, body):
        def step(i, carry):
            body(i)
            return carry
        lax.fori_loop(first, last, step, 0)

    def over_rows(c, body):
        loop(0, CHUNK // STEP, lambda i: body(pl.multiple_of(c * CHUNK + i * STEP, STEP)))

    loop(0, CHUNKS, lambda c: load(c).start())
    barrier = pltpu.get_barrier_semaphore()
    greeted = [left, right, *(p for group in partners for p in group)]
    for other in greeted:
        pl.semaphore_signal(barrier, inc=1, device_id=(other,), device_id_type=MESH)
    for j in range(TILES):
        for edge in (slice(0, PAD), slice(PAD + ROWS, 2 * PAD + ROWS)):
            for k in range(DEPTH):
                t_ref[k, j, edge, :] = jnp.zeros((PAD, LANES), jnp.float32)
            g_ref[j, edge, :] = jnp.zeros((PAD, LANES), jnp.int32)
    for k in range(3):
        tally[k] = jnp.zeros((8, LANES), jnp.int32)

    def prepare(c):
        load(c).wait()

        def body(row):
            for k in range(DEPTH):
                tiles = [x_buf[k, pl.ds(row, STEP), cols(j)] for j in range(TILES)]
                for j, t in enumerate(interleave(tiles)):
                    f_ref[2 + k, pl.ds(row, STEP), cols(j)] = embed(t)
        over_rows(c, body)

    def send_planes(c):
        prepare(c)
        start(planes(c))

    prepare(0)
    pl.semaphore_wait(barrier, len(greeted))
    start(planes(0))
    loop(1, CHUNKS, send_planes)

    def rounds(first, second, arrive, leave):
        arrive(0)
        over_rows(0, lambda row: first(row)())

        def step(c):
            arrive(c)

            def body(row):
                finish = first(row)
                second(pl.multiple_of(row - CHUNK, STEP))
                finish()
            over_rows(c, body)
            leave(c - 1)
        loop(1, CHUNKS, step)
        over_rows(CHUNKS - 1, second)
        leave(CHUNKS - 1)

    def add_count(k, flags):
        while len(flags) > 1:
            flags = [a + b for a, b in zip(flags[::2], flags[1::2])]
        tally[k] += flags[0][:8] + flags[0][8:]

    def sides_of(outs):
        return [column_sides([o[k] for o in outs]) for k in range(DEPTH)]

    def put(row, outs, sides):
        for k in range(DEPTH):
            tiles = column_window([o[k] for o in outs], sides[k], jnp.maximum)
            for j, t in enumerate(tiles):
                t_ref[k, j, pl.ds(row + PAD, STEP), :] = t

    def first1(row):
        outs, halos = [], []
        for j in range(TILES):
            at = (pl.ds(row, STEP), cols(j))
            p = [f_ref[(k,) + at] for k in range(8)]
            for k, keep in ((0, keep_lo), (1, keep_lo), (6, keep_hi), (7, keep_hi)):
                p[k] = p[k] * keep
                halos.append(((k,) + at, p[k]))
            outs.append(depth_max5(p))
        sides = sides_of(outs)

        def finish():
            for at, value in halos:
                f_ref[at] = value
            put(row, outs, sides)
        return finish

    def second1(row):
        flags = []
        for j in range(TILES):
            at = (pl.ds(row, STEP), cols(j))
            roots = []
            for k in range(DEPTH):
                s = f_ref[(2 + k,) + at]
                root = row_window(t_ref, (k, j), row, jnp.maximum) == s
                l1_ref[(k,) + at] = jnp.where(root, ROOT, s)
                flags.append(jnp.where(root, 0, 1))
                roots.append(root)
            lo = jnp.zeros((STEP, LANES), jnp.float32)
            hi = lo
            for k in range(DEPTH):
                hi = jnp.where(roots[k], float(DEPTH - k), hi)
                lo = jnp.where(roots[DEPTH - 1 - k], float(DEPTH - k), lo)
            send_lo1[at] = lo.astype(jnp.bfloat16)
            send_hi1[at] = hi.astype(jnp.bfloat16)
        add_count(0, flags)

    rounds(first1, second1, lambda c: wait_recv(planes(c)), lambda c: start(roots1(c)))

    def first2(row):
        outs, marks = [], []
        for j in range(TILES):
            at = (pl.ds(row, STEP), cols(j))
            d_lo = recv_lo1[at].astype(jnp.float32) * keep_lo
            d_hi = recv_hi1[at].astype(jnp.float32) * keep_hi
            mine = [l1_ref[(k,) + at] for k in range(DEPTH)]
            outs.append(depth_max5([
                jnp.where(d_lo == 2.0, ROOT, f_ref[(0,) + at]),
                jnp.where(d_lo == 1.0, ROOT, f_ref[(1,) + at]),
                *mine,
                jnp.where(d_hi == 1.0, ROOT, f_ref[(6,) + at]),
                jnp.where(d_hi == 2.0, ROOT, f_ref[(7,) + at]),
            ]))
            mark = jnp.where(d_lo > 3.5, 1, jnp.where(d_lo > 0.5, 3, 0))
            mark |= jnp.where(d_hi > 3.5, 8, jnp.where(d_hi > 0.5, 12, 0))
            for value, bits in zip(mine, (3, 2, 4, 12)):
                mark |= jnp.where(value == ROOT, bits, 0)
            marks.append(mark)
        sides, mark_sides = sides_of(outs), column_sides(marks)

        def finish():
            put(row, outs, sides)
            for j, t in enumerate(column_window(marks, mark_sides, jnp.bitwise_or)):
                g_ref[j, pl.ds(row + PAD, STEP), :] = t
        return finish

    def second2(row):
        flags = []
        for j in range(TILES):
            at = (pl.ds(row, STEP), cols(j))
            roots = []
            for k in range(DEPTH):
                l = l1_ref[(k,) + at]
                top = row_window(t_ref, (k, j), row, jnp.maximum)
                root, near = top == l, top >= ROOT
                value = jnp.where(root, ROOT, jnp.where(near, 0.0, l))
                l2_ref[(k,) + at] = value
                flags.append(jnp.where(root | near, 0, 1))
                roots.append(root)
            gone_ref[at] = row_window(g_ref, (j,), row, jnp.bitwise_or)
            lo = jnp.where(roots[0], 1.0, jnp.where(roots[1], 2.0, 0.0))
            hi = jnp.where(roots[3], 1.0, jnp.where(roots[2], 2.0, 0.0))
            send_lo2[at] = lo.astype(jnp.bfloat16)
            send_hi2[at] = hi.astype(jnp.bfloat16)
        add_count(1, flags)

    rounds(first2, second2, lambda c: wait_recv(roots1(c)), lambda c: start(roots2(c)))

    def first3(row):
        outs = []
        for j in range(TILES):
            at = (pl.ds(row, STEP), cols(j))
            d_lo = recv_lo2[at].astype(jnp.float32) * keep_lo
            d_hi = recv_hi2[at].astype(jnp.float32) * keep_hi
            gone = gone_ref[at]

            def halo(k, bit, is_root):
                left_over = jnp.where((gone & bit) == 0, f_ref[(k,) + at], 0.0)
                return jnp.where(is_root, ROOT, left_over)

            outs.append(depth_max5([
                halo(0, 1, d_lo == 2.0), halo(1, 2, d_lo == 1.0),
                *(l2_ref[(k,) + at] for k in range(DEPTH)),
                halo(6, 4, d_hi == 1.0), halo(7, 8, d_hi == 2.0),
            ]))
        sides = sides_of(outs)
        return lambda: put(row, outs, sides)

    def second3(row):
        flags, words = [], []
        for j in range(TILES):
            at = (pl.ds(row, STEP), cols(j))
            word = None
            for k in range(DEPTH):
                top = row_window(t_ref, (k, j), row, jnp.maximum)
                root, near = top == l2_ref[(k,) + at], top >= ROOT
                state = jnp.where(root, 1 << 2 * k, jnp.where(near, 2 << 2 * k, 0))
                word = state if word is None else word | state
                flags.append(jnp.where(root | near, 0, 1))
            words.append(word)
        for j, t in enumerate(natural(words)):
            st_ref[pl.ds(row, STEP), cols(j)] = t
        add_count(2, flags)

    rounds(first3, second3, lambda c: wait_recv(roots2(c)), lambda c: store(c).start())

    for k in range(3):
        part[0, k:k + 1, :] = jnp.sum(tally[k], axis=0, keepdims=True)
    part[0, 3:8, :] = jnp.zeros((5, LANES), jnp.int32)
    slot = 0
    for stage, group in enumerate(partners):
        copies = [
            pltpu.make_async_remote_copy(
                src_ref=part.at[stage], dst_ref=parts.at[slot + o],
                send_sem=part_send.at[slot + o], recv_sem=part_recv.at[slot + o],
                device_id=(other,), device_id_type=MESH,
            )
            for o, other in enumerate(group)
        ]
        start(copies)
        total = part[stage]
        for o, copy in enumerate(copies):
            copy.wait_recv()
            total = total + parts[slot + o]
        part[stage + 1] = total
        wait_send(copies)
        slot += len(group)
    for k in range(3):
        count_ref[k] = jnp.sum(part[len(GROUPS), k:k + 1, :])

    def drain(c):
        wait_send(planes(c))
        wait_send(roots1(c))
        wait_send(roots2(c))
        store(c).wait()

    loop(0, CHUNKS, drain)


def shards(n, scores):
    slab = (DEPTH, ROWS, COLS)
    column = pltpu.VMEM((ROWS, COLS), jnp.bfloat16)
    slots = sum(GROUPS) - len(GROUPS)
    words, counts = pl.pallas_call(
        functools.partial(kernel, n),
        out_shape=(
            jax.ShapeDtypeStruct((ROWS, COLS), jnp.int32),
            jax.ShapeDtypeStruct((3,), jnp.int32),
        ),
        in_specs=[pl.BlockSpec(memory_space=pl.ANY)],
        out_specs=(
            pl.BlockSpec(memory_space=pl.ANY),
            pl.BlockSpec(memory_space=pltpu.SMEM),
        ),
        scratch_shapes=[
            pltpu.VMEM(slab, jnp.int32),
            pltpu.VMEM((2 * DEPTH, ROWS, COLS), jnp.float32),
            pltpu.VMEM(slab, jnp.float32),
            pltpu.VMEM(slab, jnp.float32),
            pltpu.VMEM((ROWS, COLS), jnp.int32),
            pltpu.VMEM((DEPTH, TILES, ROWS + 2 * PAD, LANES), jnp.float32),
            pltpu.VMEM((TILES, ROWS + 2 * PAD, LANES), jnp.int32),
            pltpu.VMEM((ROWS, COLS), jnp.int32),
            *[column] * 8,
            pltpu.VMEM((3, 8, LANES), jnp.int32),
            pltpu.VMEM((len(GROUPS) + 1, 8, LANES), jnp.int32),
            pltpu.VMEM((slots, 8, LANES), jnp.int32),
            pltpu.SemaphoreType.DMA((CHUNKS,)),
            pltpu.SemaphoreType.DMA((CHUNKS,)),
            pltpu.SemaphoreType.DMA((3, 2, CHUNKS)),
            pltpu.SemaphoreType.DMA((3, 2, CHUNKS)),
            pltpu.SemaphoreType.DMA((slots,)),
            pltpu.SemaphoreType.DMA((slots,)),
        ],
        compiler_params=pltpu.CompilerParams(
            collective_id=0, has_side_effects=True, vmem_limit_bytes=56 << 20
        ),
    )(scores)
    plane = lax.broadcasted_iota(jnp.int32, slab, 0)
    return jnp.right_shift(jnp.right_shift(words[None], plane), plane) & 3, counts


def solution(mesh):
    n = mesh.shape["gz"]
    return jax.shard_map(
        functools.partial(shards, n),
        mesh=mesh,
        in_specs=(P("gz", None, None),),
        out_specs=(P("gz", None, None), P()),
        check_vma=False,
    )
```

```python
import functools

import jax
import jax.numpy as jnp
from jax import lax
from jax.experimental import pallas as pl
from jax.experimental.pallas import tpu as pltpu
from jax.sharding import PartitionSpec as P

DEPTH = 4
ROWS = 512
COLS = 512
LANES = 128
TILES = 4
BLOCK = LANES // TILES
CHUNK = 32
CHUNKS = ROWS // CHUNK
STEP = 16
OUT_ROWS = 256
PAD = 8
GROUPS = (8, 16)
ROOT = float(1 << 40)
MANTISSA = 23
BITS = 27
SPARE = 32 - BITS
CARRIERS = 6
SENT = 2 * TILES - 1
MESH = pl.DeviceIdType.MESH


def cols(j):
    return slice(j * LANES, (j + 1) * LANES)


def gather(x, index):
    halves = [
        jnp.take_along_axis(x[r:r + 8], index, axis=1, mode="promise_in_bounds")
        for r in range(0, x.shape[0], 8)
    ]
    return jnp.concatenate(halves, axis=0)


def lane_of(height):
    return lax.broadcasted_iota(jnp.int32, (height, LANES), 1)


def by_block(tiles, source):
    block = lane_of(tiles[0].shape[0]) // BLOCK
    out = []
    for a in range(TILES):
        t = tiles[source(TILES - 1, a)]
        for p in range(TILES - 1):
            t = jnp.where(block == p, tiles[source(p, a)], t)
        out.append(t)
    return out


def interleave(tiles):
    lane = lane_of(8)
    sorted_ = [
        gather(t, (lane % BLOCK) * TILES + (lane // BLOCK + TILES - s) % TILES)
        for s, t in enumerate(tiles)
    ]
    mixed = by_block(sorted_, lambda p, j: (p - j) % TILES)
    return [pltpu.roll(t, LANES - BLOCK * j, 1) if j else t for j, t in enumerate(mixed)]


def natural(tiles):
    lane = lane_of(8)
    turned = [pltpu.roll(t, BLOCK * j, 1) if j else t for j, t in enumerate(tiles)]
    mixed = by_block(turned, lambda p, s: (p - s) % TILES)
    return [
        gather(t, BLOCK * ((lane % TILES + s) % TILES) + lane // TILES)
        for s, t in enumerate(mixed)
    ]


def column_sides(t):
    lane = lane_of(t[0].shape[0])
    zero = jnp.zeros(t[0].shape, t[0].dtype)
    before = [jnp.where(lane == 0, zero, pltpu.roll(t[j], 1, 1)) for j in (2, 3)]
    after = [jnp.where(lane == LANES - 1, zero, pltpu.roll(t[j], LANES - 1, 1)) for j in (0, 1)]
    return (*before, *after)


def column_window(t, sides, join):
    r2, r3, l0, l1 = sides
    m12 = join(t[1], t[2])
    m012, m123 = join(t[0], m12), join(m12, t[3])
    whole = join(m012, t[3])
    return [join(m012, join(r2, r3)), join(whole, r3), join(whole, l0), join(m123, join(l0, l1))]


def depth_max5(p):
    m34 = jnp.maximum(p[3], p[4])
    a = jnp.maximum(p[2], m34)
    a5 = jnp.maximum(a, p[5])
    return [
        jnp.maximum(jnp.maximum(p[0], p[1]), a),
        jnp.maximum(p[1], a5),
        jnp.maximum(a5, p[6]),
        jnp.maximum(jnp.maximum(m34, p[5]), jnp.maximum(p[6], p[7])),
    ]


def row_window(ref, at, row, join):
    parts = [ref[(*at, pl.ds(row + PAD + d, STEP), slice(None))] for d in (-2, -1, 0, 1, 2)]
    return join(join(join(parts[0], parts[1]), join(parts[3], parts[4])), parts[2])


def embed(s):
    low = (s & ((1 << MANTISSA) - 1)) | (1 << MANTISSA)
    exponent = jnp.right_shift(s, MANTISSA) & ((1 << (BITS - MANTISSA)) - 1)
    return low.astype(jnp.float32) * jnp.left_shift(jnp.ones_like(s), exponent).astype(jnp.float32)


def pack(tiles):
    *words, spare = tiles
    for i in range(CARRIERS):
        words[i] = words[i] | jnp.left_shift(jnp.right_shift(spare, SPARE * i), BITS)
    return words


def unpack(words):
    spare = None
    for i in range(CARRIERS):
        bits = jnp.left_shift(lax.shift_right_logical(words[i], BITS), SPARE * i)
        spare = bits if spare is None else spare | bits
    return [*words, spare]


def kernel(
    n, x_ref, out_ref, count_ref,
    x_buf, f_ref, l1_ref, l2_ref, gone_ref, t_ref, g_ref, st_ref,
    send_lo1, send_hi1, recv_lo1, recv_hi1, send_lo2, send_hi2, recv_lo2, recv_hi2,
    pack_lo, pack_hi, packed_lo, packed_hi, tally, part, parts,
    load_sem, store_sem, send_sems, recv_sems, part_send, part_recv,
):
    me = lax.axis_index("gz")
    right, left = lax.rem(me + 1, n), lax.rem(me + n - 1, n)
    keep_lo = jnp.where(me > 0, 1.0, 0.0).astype(jnp.float32)
    keep_hi = jnp.where(me < n - 1, 1.0, 0.0).astype(jnp.float32)

    partners = []
    stride = 1
    for size in GROUPS:
        place = lax.rem(lax.div(me, stride), size)
        partners.append(
            [me + (lax.rem(place + o, size) - place) * stride for o in range(1, size)]
        )
        stride *= size

    def rows_of(c):
        return pl.ds(pl.multiple_of(c * CHUNK, CHUNK), CHUNK)

    def load(c):
        return pltpu.make_async_copy(
            x_ref.at[:, rows_of(c), :], x_buf.at[:, rows_of(c), :], load_sem.at[c]
        )

    def store(c):
        return pltpu.make_async_copy(
            st_ref.at[rows_of(c), :], out_ref.at[rows_of(c), :], store_sem.at[c]
        )

    def remote(src, dst, stage, side, c, device):
        return pltpu.make_async_remote_copy(
            src_ref=src, dst_ref=dst,
            send_sem=send_sems.at[stage, side, c], recv_sem=recv_sems.at[stage, side, c],
            device_id=(device,), device_id_type=MESH,
        )

    def planes(c):
        r = rows_of(c)
        return (
            remote(pack_lo.at[r, :], packed_hi.at[r, :], 0, 1, c, left),
            remote(pack_hi.at[r, :], packed_lo.at[r, :], 0, 0, c, right),
        )

    def roots1(c):
        r = rows_of(c)
        return (
            remote(send_lo1.at[r, :], recv_hi1.at[r, :], 1, 1, c, left),
            remote(send_hi1.at[r, :], recv_lo1.at[r, :], 1, 0, c, right),
        )

    def roots2(c):
        r = rows_of(c)
        return (
            remote(send_lo2.at[r, :], recv_hi2.at[r, :], 2, 1, c, left),
            remote(send_hi2.at[r, :], recv_lo2.at[r, :], 2, 0, c, right),
        )

    def start(pair):
        for copy in pair:
            copy.start()

    def wait_recv(pair):
        for copy in pair:
            copy.wait_recv()

    def wait_send(pair):
        for copy in pair:
            copy.wait_send()

    def loop(first, last, body):
        def step(i, carry):
            body(i)
            return carry
        lax.fori_loop(first, last, step, 0)

    def over_rows(c, body):
        loop(0, CHUNK // STEP, lambda i: body(pl.multiple_of(c * CHUNK + i * STEP, STEP)))

    loop(0, CHUNKS, lambda c: load(c).start())
    barrier = pltpu.get_barrier_semaphore()
    greeted = [left, right, *(p for group in partners for p in group)]
    for other in greeted:
        pl.semaphore_signal(barrier, inc=1, device_id=(other,), device_id_type=MESH)
    for j in range(TILES):
        for edge in (slice(0, PAD), slice(PAD + ROWS, 2 * PAD + ROWS)):
            for k in range(DEPTH):
                t_ref[k, j, edge, :] = jnp.zeros((PAD, LANES), jnp.float32)
            g_ref[j, edge, :] = jnp.zeros((PAD, LANES), jnp.int32)
    for k in range(3):
        tally[k] = jnp.zeros((8, LANES), jnp.int32)

    def prepare(c):
        load(c).wait()

        def body(row):
            own = []
            for k in range(DEPTH):
                tiles = [x_buf[k, pl.ds(row, STEP), cols(j)] for j in range(TILES)]
                own += interleave(tiles)
            for ref, tiles in ((pack_lo, own[:2 * TILES]), (pack_hi, own[2 * TILES:])):
                for i, word in enumerate(pack(tiles)):
                    ref[pl.ds(row, STEP), cols(i)] = word
            for i, t in enumerate(own):
                f_ref[2 + i // TILES, pl.ds(row, STEP), cols(i % TILES)] = embed(t)
        over_rows(c, body)

    def send_planes(c):
        prepare(c)
        start(planes(c))

    prepare(0)
    pl.semaphore_wait(barrier, len(greeted))
    start(planes(0))
    loop(1, CHUNKS, send_planes)

    def rounds(first, second, arrive, leave):
        arrive(0)
        over_rows(0, lambda row: first(row)())

        def step(c):
            arrive(c)

            def body(row):
                finish = first(row)
                second(pl.multiple_of(row - CHUNK, STEP))
                finish()
            over_rows(c, body)
            leave(c - 1)
        loop(1, CHUNKS, step)
        over_rows(CHUNKS - 1, second)
        leave(CHUNKS - 1)

    def add_count(k, flags):
        while len(flags) > 1:
            flags = [a + b for a, b in zip(flags[::2], flags[1::2])]
        tally[k] += flags[0][:8] + flags[0][8:]

    def sides_of(outs):
        return [column_sides([o[k] for o in outs]) for k in range(DEPTH)]

    def put(row, outs, sides):
        for k in range(DEPTH):
            tiles = column_window([o[k] for o in outs], sides[k], jnp.maximum)
            for j, t in enumerate(tiles):
                t_ref[k, j, pl.ds(row + PAD, STEP), :] = t

    def first1(row):
        outs, halos = [], []
        rows = pl.ds(row, STEP)
        low, high = (
            [embed(t) * keep for t in unpack([ref[rows, cols(i)] for i in range(SENT)])]
            for ref, keep in ((packed_lo, keep_lo), (packed_hi, keep_hi))
        )
        for j in range(TILES):
            at = (rows, cols(j))
            p = [
                low[j], low[TILES + j], *(f_ref[(k,) + at] for k in range(2, 6)),
                high[j], high[TILES + j],
            ]
            halos += [((k,) + at, p[k]) for k in (0, 1, 6, 7)]
            outs.append(depth_max5(p))
        sides = sides_of(outs)

        def finish():
            for at, value in halos:
                f_ref[at] = value
            put(row, outs, sides)
        return finish

    def second1(row):
        flags = []
        for j in range(TILES):
            at = (pl.ds(row, STEP), cols(j))
            roots = []
            for k in range(DEPTH):
                s = f_ref[(2 + k,) + at]
                root = row_window(t_ref, (k, j), row, jnp.maximum) == s
                l1_ref[(k,) + at] = jnp.where(root, ROOT, s)
                flags.append(jnp.where(root, 0, 1))
                roots.append(root)
            lo = jnp.zeros((STEP, LANES), jnp.float32)
            hi = lo
            for k in range(DEPTH):
                hi = jnp.where(roots[k], float(DEPTH - k), hi)
                lo = jnp.where(roots[DEPTH - 1 - k], float(DEPTH - k), lo)
            send_lo1[at] = lo.astype(jnp.bfloat16)
            send_hi1[at] = hi.astype(jnp.bfloat16)
        add_count(0, flags)

    rounds(first1, second1, lambda c: wait_recv(planes(c)), lambda c: start(roots1(c)))

    def first2(row):
        outs, marks = [], []
        for j in range(TILES):
            at = (pl.ds(row, STEP), cols(j))
            d_lo = recv_lo1[at].astype(jnp.float32) * keep_lo
            d_hi = recv_hi1[at].astype(jnp.float32) * keep_hi
            mine = [l1_ref[(k,) + at] for k in range(DEPTH)]
            outs.append(depth_max5([
                jnp.where(d_lo == 2.0, ROOT, f_ref[(0,) + at]),
                jnp.where(d_lo == 1.0, ROOT, f_ref[(1,) + at]),
                *mine,
                jnp.where(d_hi == 1.0, ROOT, f_ref[(6,) + at]),
                jnp.where(d_hi == 2.0, ROOT, f_ref[(7,) + at]),
            ]))
            mark = jnp.where(d_lo > 3.5, 1, jnp.where(d_lo > 0.5, 3, 0))
            mark |= jnp.where(d_hi > 3.5, 8, jnp.where(d_hi > 0.5, 12, 0))
            for value, bits in zip(mine, (3, 2, 4, 12)):
                mark |= jnp.where(value == ROOT, bits, 0)
            marks.append(mark)
        sides, mark_sides = sides_of(outs), column_sides(marks)

        def finish():
            put(row, outs, sides)
            for j, t in enumerate(column_window(marks, mark_sides, jnp.bitwise_or)):
                g_ref[j, pl.ds(row + PAD, STEP), :] = t
        return finish

    def second2(row):
        flags = []
        for j in range(TILES):
            at = (pl.ds(row, STEP), cols(j))
            roots = []
            for k in range(DEPTH):
                l = l1_ref[(k,) + at]
                top = row_window(t_ref, (k, j), row, jnp.maximum)
                root, near = top == l, top >= ROOT
                value = jnp.where(root, ROOT, jnp.where(near, 0.0, l))
                l2_ref[(k,) + at] = value
                flags.append(jnp.where(root | near, 0, 1))
                roots.append(root)
            gone_ref[at] = row_window(g_ref, (j,), row, jnp.bitwise_or)
            lo = jnp.where(roots[0], 1.0, jnp.where(roots[1], 2.0, 0.0))
            hi = jnp.where(roots[3], 1.0, jnp.where(roots[2], 2.0, 0.0))
            send_lo2[at] = lo.astype(jnp.bfloat16)
            send_hi2[at] = hi.astype(jnp.bfloat16)
        add_count(1, flags)

    rounds(first2, second2, lambda c: wait_recv(roots1(c)), lambda c: start(roots2(c)))

    def first3(row):
        outs = []
        for j in range(TILES):
            at = (pl.ds(row, STEP), cols(j))
            d_lo = recv_lo2[at].astype(jnp.float32) * keep_lo
            d_hi = recv_hi2[at].astype(jnp.float32) * keep_hi
            gone = gone_ref[at]

            def halo(k, bit, is_root):
                left_over = jnp.where((gone & bit) == 0, f_ref[(k,) + at], 0.0)
                return jnp.where(is_root, ROOT, left_over)

            outs.append(depth_max5([
                halo(0, 1, d_lo == 2.0), halo(1, 2, d_lo == 1.0),
                *(l2_ref[(k,) + at] for k in range(DEPTH)),
                halo(6, 4, d_hi == 1.0), halo(7, 8, d_hi == 2.0),
            ]))
        sides = sides_of(outs)
        return lambda: put(row, outs, sides)

    def second3(row):
        flags, words = [], []
        for j in range(TILES):
            at = (pl.ds(row, STEP), cols(j))
            word = None
            for k in range(DEPTH):
                top = row_window(t_ref, (k, j), row, jnp.maximum)
                root, near = top == l2_ref[(k,) + at], top >= ROOT
                state = jnp.where(root, 1 << 2 * k, jnp.where(near, 2 << 2 * k, 0))
                word = state if word is None else word | state
                flags.append(jnp.where(root | near, 0, 1))
            words.append(word)
        for j, t in enumerate(natural(words)):
            st_ref[pl.ds(row, STEP), cols(j)] = t
        add_count(2, flags)

    rounds(first3, second3, lambda c: wait_recv(roots2(c)), lambda c: store(c).start())

    for k in range(3):
        part[0, k:k + 1, :] = jnp.sum(tally[k], axis=0, keepdims=True)
    part[0, 3:8, :] = jnp.zeros((5, LANES), jnp.int32)
    slot = 0
    for stage, group in enumerate(partners):
        copies = [
            pltpu.make_async_remote_copy(
                src_ref=part.at[stage], dst_ref=parts.at[slot + o],
                send_sem=part_send.at[slot + o], recv_sem=part_recv.at[slot + o],
                device_id=(other,), device_id_type=MESH,
            )
            for o, other in enumerate(group)
        ]
        start(copies)
        total = part[stage]
        for o, copy in enumerate(copies):
            copy.wait_recv()
            total = total + parts[slot + o]
        part[stage + 1] = total
        wait_send(copies)
        slot += len(group)
    for k in range(3):
        count_ref[k] = jnp.sum(part[len(GROUPS), k:k + 1, :])

    def drain(c):
        wait_send(planes(c))
        wait_send(roots1(c))
        wait_send(roots2(c))
        store(c).wait()

    loop(0, CHUNKS, drain)


def expand(word_ref, count_ref, out_ref, count_out_ref):
    words = word_ref[...]
    for k in range(DEPTH):
        out_ref[k] = jnp.right_shift(words, 2 * k) & 3
    for k in range(3):
        count_out_ref[k] = count_ref[k]


def shards(n, scores):
    slab = (DEPTH, ROWS, COLS)
    column = pltpu.VMEM((ROWS, COLS), jnp.bfloat16)
    slots = sum(GROUPS) - len(GROUPS)
    words, counts = pl.pallas_call(
        functools.partial(kernel, n),
        out_shape=(
            jax.ShapeDtypeStruct((ROWS, COLS), jnp.int32),
            jax.ShapeDtypeStruct((3,), jnp.int32),
        ),
        in_specs=[pl.BlockSpec(memory_space=pl.ANY)],
        out_specs=(
            pl.BlockSpec(memory_space=pl.ANY),
            pl.BlockSpec(memory_space=pltpu.SMEM),
        ),
        scratch_shapes=[
            pltpu.VMEM(slab, jnp.int32),
            pltpu.VMEM((2 * DEPTH, ROWS, COLS), jnp.float32),
            pltpu.VMEM(slab, jnp.float32),
            pltpu.VMEM(slab, jnp.float32),
            pltpu.VMEM((ROWS, COLS), jnp.int32),
            pltpu.VMEM((DEPTH, TILES, ROWS + 2 * PAD, LANES), jnp.float32),
            pltpu.VMEM((TILES, ROWS + 2 * PAD, LANES), jnp.int32),
            pltpu.VMEM((ROWS, COLS), jnp.int32),
            *[column] * 8,
            *[pltpu.VMEM((ROWS, SENT * LANES), jnp.int32)] * 4,
            pltpu.VMEM((3, 8, LANES), jnp.int32),
            pltpu.VMEM((len(GROUPS) + 1, 8, LANES), jnp.int32),
            pltpu.VMEM((slots, 8, LANES), jnp.int32),
            pltpu.SemaphoreType.DMA((CHUNKS,)),
            pltpu.SemaphoreType.DMA((CHUNKS,)),
            pltpu.SemaphoreType.DMA((3, 2, CHUNKS)),
            pltpu.SemaphoreType.DMA((3, 2, CHUNKS)),
            pltpu.SemaphoreType.DMA((slots,)),
            pltpu.SemaphoreType.DMA((slots,)),
        ],
        compiler_params=pltpu.CompilerParams(
            collective_id=0, has_side_effects=True, vmem_limit_bytes=56 << 20
        ),
    )(scores)
    return pl.pallas_call(
        expand,
        out_shape=(
            jax.ShapeDtypeStruct(slab, jnp.int32),
            jax.ShapeDtypeStruct((3,), jnp.int32),
        ),
        grid=(ROWS // OUT_ROWS,),
        in_specs=[
            pl.BlockSpec((OUT_ROWS, COLS), lambda i: (i, 0)),
            pl.BlockSpec(memory_space=pltpu.SMEM),
        ],
        out_specs=(
            pl.BlockSpec((DEPTH, OUT_ROWS, COLS), lambda i: (0, i, 0)),
            pl.BlockSpec(memory_space=pltpu.SMEM),
        ),
    )(words, counts)


def solution(mesh):
    n = mesh.shape["gz"]
    return jax.shard_map(
        functools.partial(shards, n),
        mesh=mesh,
        in_specs=(P("gz", None, None),),
        out_specs=(P("gz", None, None), P()),
        check_vma=False,
    )
```

```python
import functools

import jax
import jax.numpy as jnp
from jax import lax
from jax.experimental import pallas as pl
from jax.experimental.pallas import tpu as pltpu
from jax.sharding import PartitionSpec as P

DEPTH = 4
ROWS = 512
COLS = 512
LANES = 128
TILES = 4
BLOCK = LANES // TILES
CHUNK = 32
CHUNKS = ROWS // CHUNK
STEP = 16
OUT_ROWS = 256
PAD = 8
GROUPS = (8, 16)
ROOT = float(1 << 40)
MANTISSA = 23
BITS = 27
SPARE = 32 - BITS
CARRIERS = 6
SENT = 2 * TILES - 1
MESH = pl.DeviceIdType.MESH


def cols(j):
    return slice(j * LANES, (j + 1) * LANES)


def gather(x, index):
    halves = [
        jnp.take_along_axis(x[r:r + 8], index, axis=1, mode="promise_in_bounds")
        for r in range(0, x.shape[0], 8)
    ]
    return jnp.concatenate(halves, axis=0)


def lane_of(height):
    return lax.broadcasted_iota(jnp.int32, (height, LANES), 1)


def by_block(tiles, source):
    block = lane_of(tiles[0].shape[0]) // BLOCK
    out = []
    for a in range(TILES):
        t = tiles[source(TILES - 1, a)]
        for p in range(TILES - 1):
            t = jnp.where(block == p, tiles[source(p, a)], t)
        out.append(t)
    return out


def interleave(tiles):
    lane = lane_of(8)
    sorted_ = [
        gather(t, (lane % BLOCK) * TILES + (lane // BLOCK + TILES - s) % TILES)
        for s, t in enumerate(tiles)
    ]
    mixed = by_block(sorted_, lambda p, j: (p - j) % TILES)
    return [pltpu.roll(t, LANES - BLOCK * j, 1) if j else t for j, t in enumerate(mixed)]


def natural(tiles):
    lane = lane_of(8)
    turned = [pltpu.roll(t, BLOCK * j, 1) if j else t for j, t in enumerate(tiles)]
    mixed = by_block(turned, lambda p, s: (p - s) % TILES)
    return [
        gather(t, BLOCK * ((lane % TILES + s) % TILES) + lane // TILES)
        for s, t in enumerate(mixed)
    ]


def column_sides(t):
    lane = lane_of(t[0].shape[0])
    zero = jnp.zeros(t[0].shape, t[0].dtype)
    before = [jnp.where(lane == 0, zero, pltpu.roll(t[j], 1, 1)) for j in (2, 3)]
    after = [jnp.where(lane == LANES - 1, zero, pltpu.roll(t[j], LANES - 1, 1)) for j in (0, 1)]
    return (*before, *after)


def column_window(t, sides, join):
    r2, r3, l0, l1 = sides
    m12 = join(t[1], t[2])
    m012, m123 = join(t[0], m12), join(m12, t[3])
    whole = join(m012, t[3])
    return [join(m012, join(r2, r3)), join(whole, r3), join(whole, l0), join(m123, join(l0, l1))]


def depth_max5(p):
    m34 = jnp.maximum(p[3], p[4])
    a = jnp.maximum(p[2], m34)
    a5 = jnp.maximum(a, p[5])
    return [
        jnp.maximum(jnp.maximum(p[0], p[1]), a),
        jnp.maximum(p[1], a5),
        jnp.maximum(a5, p[6]),
        jnp.maximum(jnp.maximum(m34, p[5]), jnp.maximum(p[6], p[7])),
    ]


def row_window(ref, at, row, join):
    parts = [ref[(*at, pl.ds(row + PAD + d, STEP), slice(None))] for d in (-2, -1, 0, 1, 2)]
    return join(join(join(parts[0], parts[1]), join(parts[3], parts[4])), parts[2])


def embed(s):
    low = (s & ((1 << MANTISSA) - 1)) | (1 << MANTISSA)
    exponent = jnp.right_shift(s, MANTISSA) & ((1 << (BITS - MANTISSA)) - 1)
    return low.astype(jnp.float32) * jnp.left_shift(jnp.ones_like(s), exponent).astype(jnp.float32)


def pack(tiles):
    *words, spare = tiles
    for i in range(CARRIERS):
        words[i] = words[i] | jnp.left_shift(jnp.right_shift(spare, SPARE * i), BITS)
    return words


def unpack(words):
    spare = None
    for i in range(CARRIERS):
        bits = jnp.left_shift(lax.shift_right_logical(words[i], BITS), SPARE * i)
        spare = bits if spare is None else spare | bits
    return [*words, spare]


def kernel(
    n, x_ref, out_ref, count_ref,
    x_buf, f_ref, l1_ref, l2_ref, gone_ref, t_ref, g_ref, st_ref,
    send_lo1, send_hi1, recv_lo1, recv_hi1, send_lo2, send_hi2, recv_lo2, recv_hi2,
    pack_lo, pack_hi, packed_lo, packed_hi, tally, part, parts,
    load_sem, store_sem, send_sems, recv_sems, part_send, part_recv,
):
    me = lax.axis_index("gz")
    right, left = lax.rem(me + 1, n), lax.rem(me + n - 1, n)
    has_left, has_right = me > 0, me < n - 1

    partners = []
    stride = 1
    for size in GROUPS:
        place = lax.rem(lax.div(me, stride), size)
        partners.append(
            [me + (lax.rem(place + o, size) - place) * stride for o in range(1, size)]
        )
        stride *= size

    def rows_of(c):
        return pl.ds(pl.multiple_of(c * CHUNK, CHUNK), CHUNK)

    def load(c):
        return pltpu.make_async_copy(
            x_ref.at[:, rows_of(c), :], x_buf.at[:, rows_of(c), :], load_sem.at[c]
        )

    def store(c):
        return pltpu.make_async_copy(
            st_ref.at[rows_of(c), :], out_ref.at[rows_of(c), :], store_sem.at[c]
        )

    def remote(src, dst, stage, side, c, device):
        return pltpu.make_async_remote_copy(
            src_ref=src, dst_ref=dst,
            send_sem=send_sems.at[stage, side, c], recv_sem=recv_sems.at[stage, side, c],
            device_id=(device,), device_id_type=MESH,
        )

    def planes(c):
        r = rows_of(c)
        return (
            remote(pack_lo.at[r, :], packed_hi.at[r, :], 0, 1, c, left),
            remote(pack_hi.at[r, :], packed_lo.at[r, :], 0, 0, c, right),
        )

    def roots1(c):
        r = rows_of(c)
        return (
            remote(send_lo1.at[r, :], recv_hi1.at[r, :], 1, 1, c, left),
            remote(send_hi1.at[r, :], recv_lo1.at[r, :], 1, 0, c, right),
        )

    def roots2(c):
        r = rows_of(c)
        return (
            remote(send_lo2.at[r, :], recv_hi2.at[r, :], 2, 1, c, left),
            remote(send_hi2.at[r, :], recv_lo2.at[r, :], 2, 0, c, right),
        )

    def sided(on_left, on_right):
        pl.when(has_left)(on_left)
        pl.when(has_right)(on_right)

    def start(pair):
        sided(pair[0].start, pair[1].start)

    def wait_recv(pair):
        sided(pair[1].wait_recv, pair[0].wait_recv)

    def wait_send(pair):
        sided(pair[0].wait_send, pair[1].wait_send)

    def loop(first, last, body):
        def step(i, carry):
            body(i)
            return carry
        lax.fori_loop(first, last, step, 0)

    def over_rows(c, body):
        loop(0, CHUNK // STEP, lambda i: body(pl.multiple_of(c * CHUNK + i * STEP, STEP)))

    loop(0, CHUNKS, lambda c: load(c).start())
    barrier = pltpu.get_barrier_semaphore()

    def greet(other):
        pl.semaphore_signal(barrier, inc=1, device_id=(other,), device_id_type=MESH)

    sided(lambda: greet(left), lambda: greet(right))
    greeted = [p for group in partners for p in group]
    for other in greeted:
        greet(other)

    def outside(*refs):
        def fill():
            def body(i):
                rows = pl.ds(pl.multiple_of(i * CHUNK, CHUNK), CHUNK)
                for ref in refs:
                    ref[rows, :] = jnp.zeros((CHUNK, ref.shape[1]), ref.dtype)
            loop(0, CHUNKS, body)
        return fill

    pl.when(jnp.logical_not(has_left))(outside(packed_lo, recv_lo1, recv_lo2))
    pl.when(jnp.logical_not(has_right))(outside(packed_hi, recv_hi1, recv_hi2))
    for j in range(TILES):
        for edge in (slice(0, PAD), slice(PAD + ROWS, 2 * PAD + ROWS)):
            for k in range(DEPTH):
                t_ref[k, j, edge, :] = jnp.zeros((PAD, LANES), jnp.float32)
            g_ref[j, edge, :] = jnp.zeros((PAD, LANES), jnp.int32)
    for k in range(3):
        tally[k] = jnp.zeros((8, LANES), jnp.int32)

    def prepare(c):
        load(c).wait()

        def body(row):
            own = []
            for k in range(DEPTH):
                tiles = [x_buf[k, pl.ds(row, STEP), cols(j)] for j in range(TILES)]
                own += interleave(tiles)
            for ref, tiles in ((pack_lo, own[:2 * TILES]), (pack_hi, own[2 * TILES:])):
                for i, word in enumerate(pack(tiles)):
                    ref[pl.ds(row, STEP), cols(i)] = word
            for i, t in enumerate(own):
                f_ref[2 + i // TILES, pl.ds(row, STEP), cols(i % TILES)] = embed(t)
        over_rows(c, body)

    def send_planes(c):
        prepare(c)
        start(planes(c))

    prepare(0)
    neighbours = has_left.astype(jnp.int32) + has_right.astype(jnp.int32)
    pl.semaphore_wait(barrier, neighbours + len(greeted))
    start(planes(0))
    loop(1, CHUNKS, send_planes)

    def rounds(first, second, arrive, leave):
        arrive(0)
        over_rows(0, lambda row: first(row)())

        def step(c):
            arrive(c)

            def body(row):
                finish = first(row)
                second(pl.multiple_of(row - CHUNK, STEP))
                finish()
            over_rows(c, body)
            leave(c - 1)
        loop(1, CHUNKS, step)
        over_rows(CHUNKS - 1, second)
        leave(CHUNKS - 1)

    def add_count(k, flags):
        while len(flags) > 1:
            flags = [a + b for a, b in zip(flags[::2], flags[1::2])]
        tally[k] += flags[0][:8] + flags[0][8:]

    def sides_of(outs):
        return [column_sides([o[k] for o in outs]) for k in range(DEPTH)]

    def put(row, outs, sides):
        for k in range(DEPTH):
            tiles = column_window([o[k] for o in outs], sides[k], jnp.maximum)
            for j, t in enumerate(tiles):
                t_ref[k, j, pl.ds(row + PAD, STEP), :] = t

    def first1(row):
        outs, halos = [], []
        rows = pl.ds(row, STEP)
        low, high = (
            [embed(t) for t in unpack([ref[rows, cols(i)] for i in range(SENT)])]
            for ref in (packed_lo, packed_hi)
        )
        for j in range(TILES):
            at = (rows, cols(j))
            p = [
                low[j], low[TILES + j], *(f_ref[(k,) + at] for k in range(2, 6)),
                high[j], high[TILES + j],
            ]
            halos += [((k,) + at, p[k]) for k in (0, 1, 6, 7)]
            outs.append(depth_max5(p))
        sides = sides_of(outs)

        def finish():
            for at, value in halos:
                f_ref[at] = value
            put(row, outs, sides)
        return finish

    def second1(row):
        flags = []
        for j in range(TILES):
            at = (pl.ds(row, STEP), cols(j))
            roots = []
            for k in range(DEPTH):
                s = f_ref[(2 + k,) + at]
                root = row_window(t_ref, (k, j), row, jnp.maximum) == s
                l1_ref[(k,) + at] = jnp.where(root, ROOT, s)
                flags.append(jnp.where(root, 0, 1))
                roots.append(root)
            lo = jnp.zeros((STEP, LANES), jnp.float32)
            hi = lo
            for k in range(DEPTH):
                hi = jnp.where(roots[k], float(DEPTH - k), hi)
                lo = jnp.where(roots[DEPTH - 1 - k], float(DEPTH - k), lo)
            send_lo1[at] = lo.astype(jnp.bfloat16)
            send_hi1[at] = hi.astype(jnp.bfloat16)
        add_count(0, flags)

    rounds(first1, second1, lambda c: wait_recv(planes(c)), lambda c: start(roots1(c)))

    def first2(row):
        outs, marks = [], []
        for j in range(TILES):
            at = (pl.ds(row, STEP), cols(j))
            d_lo = recv_lo1[at].astype(jnp.float32)
            d_hi = recv_hi1[at].astype(jnp.float32)
            mine = [l1_ref[(k,) + at] for k in range(DEPTH)]
            outs.append(depth_max5([
                jnp.where(d_lo == 2.0, ROOT, f_ref[(0,) + at]),
                jnp.where(d_lo == 1.0, ROOT, f_ref[(1,) + at]),
                *mine,
                jnp.where(d_hi == 1.0, ROOT, f_ref[(6,) + at]),
                jnp.where(d_hi == 2.0, ROOT, f_ref[(7,) + at]),
            ]))
            mark = jnp.where(d_lo > 3.5, 1, jnp.where(d_lo > 0.5, 3, 0))
            mark |= jnp.where(d_hi > 3.5, 8, jnp.where(d_hi > 0.5, 12, 0))
            for value, bits in zip(mine, (3, 2, 4, 12)):
                mark |= jnp.where(value == ROOT, bits, 0)
            marks.append(mark)
        sides, mark_sides = sides_of(outs), column_sides(marks)

        def finish():
            put(row, outs, sides)
            for j, t in enumerate(column_window(marks, mark_sides, jnp.bitwise_or)):
                g_ref[j, pl.ds(row + PAD, STEP), :] = t
        return finish

    def second2(row):
        flags = []
        for j in range(TILES):
            at = (pl.ds(row, STEP), cols(j))
            roots = []
            for k in range(DEPTH):
                l = l1_ref[(k,) + at]
                top = row_window(t_ref, (k, j), row, jnp.maximum)
                root, near = top == l, top >= ROOT
                value = jnp.where(root, ROOT, jnp.where(near, 0.0, l))
                l2_ref[(k,) + at] = value
                flags.append(jnp.where(root | near, 0, 1))
                roots.append(root)
            gone_ref[at] = row_window(g_ref, (j,), row, jnp.bitwise_or)
            lo = jnp.where(roots[0], 1.0, jnp.where(roots[1], 2.0, 0.0))
            hi = jnp.where(roots[3], 1.0, jnp.where(roots[2], 2.0, 0.0))
            send_lo2[at] = lo.astype(jnp.bfloat16)
            send_hi2[at] = hi.astype(jnp.bfloat16)
        add_count(1, flags)

    rounds(first2, second2, lambda c: wait_recv(roots1(c)), lambda c: start(roots2(c)))

    def first3(row):
        outs = []
        for j in range(TILES):
            at = (pl.ds(row, STEP), cols(j))
            d_lo = recv_lo2[at].astype(jnp.float32)
            d_hi = recv_hi2[at].astype(jnp.float32)
            gone = gone_ref[at]

            def halo(k, bit, is_root):
                left_over = jnp.where((gone & bit) == 0, f_ref[(k,) + at], 0.0)
                return jnp.where(is_root, ROOT, left_over)

            outs.append(depth_max5([
                halo(0, 1, d_lo == 2.0), halo(1, 2, d_lo == 1.0),
                *(l2_ref[(k,) + at] for k in range(DEPTH)),
                halo(6, 4, d_hi == 1.0), halo(7, 8, d_hi == 2.0),
            ]))
        sides = sides_of(outs)
        return lambda: put(row, outs, sides)

    def second3(row):
        flags = []
        for j in range(TILES):
            at = (pl.ds(row, STEP), cols(j))
            word = None
            for k in range(DEPTH):
                top = row_window(t_ref, (k, j), row, jnp.maximum)
                root, near = top == l2_ref[(k,) + at], top >= ROOT
                state = jnp.where(root, 1 << 2 * k, jnp.where(near, 2 << 2 * k, 0))
                word = state if word is None else word | state
                flags.append(jnp.where(root | near, 0, 1))
            st_ref[at] = word
        add_count(2, flags)

    rounds(first3, second3, lambda c: wait_recv(roots2(c)), lambda c: store(c).start())

    for k in range(3):
        part[0, k:k + 1, :] = jnp.sum(tally[k], axis=0, keepdims=True)
    part[0, 3:8, :] = jnp.zeros((5, LANES), jnp.int32)
    slot = 0
    for stage, group in enumerate(partners):
        copies = [
            pltpu.make_async_remote_copy(
                src_ref=part.at[stage], dst_ref=parts.at[slot + o],
                send_sem=part_send.at[slot + o], recv_sem=part_recv.at[slot + o],
                device_id=(other,), device_id_type=MESH,
            )
            for o, other in enumerate(group)
        ]
        for copy in copies:
            copy.start()
        total = part[stage]
        for o, copy in enumerate(copies):
            copy.wait_recv()
            total = total + parts[slot + o]
        part[stage + 1] = total
        for copy in copies:
            copy.wait_send()
        slot += len(group)
    for k in range(3):
        count_ref[k] = jnp.sum(part[len(GROUPS), k:k + 1, :])

    def drain(c):
        wait_send(planes(c))
        wait_send(roots1(c))
        wait_send(roots2(c))
        store(c).wait()

    loop(0, CHUNKS, drain)


def expand(word_ref, count_ref, out_ref, count_out_ref):
    for j, words in enumerate(natural([word_ref[:, cols(j)] for j in range(TILES)])):
        for k in range(DEPTH):
            out_ref[k, :, cols(j)] = jnp.right_shift(words, 2 * k) & 3
    for k in range(3):
        count_out_ref[k] = count_ref[k]


def shards(n, scores):
    slab = (DEPTH, ROWS, COLS)
    column = pltpu.VMEM((ROWS, COLS), jnp.bfloat16)
    slots = sum(GROUPS) - len(GROUPS)
    words, counts = pl.pallas_call(
        functools.partial(kernel, n),
        out_shape=(
            jax.ShapeDtypeStruct((ROWS, COLS), jnp.int32),
            jax.ShapeDtypeStruct((3,), jnp.int32),
        ),
        in_specs=[pl.BlockSpec(memory_space=pl.ANY)],
        out_specs=(
            pl.BlockSpec(memory_space=pl.ANY),
            pl.BlockSpec(memory_space=pltpu.SMEM),
        ),
        scratch_shapes=[
            pltpu.VMEM(slab, jnp.int32),
            pltpu.VMEM((2 * DEPTH, ROWS, COLS), jnp.float32),
            pltpu.VMEM(slab, jnp.float32),
            pltpu.VMEM(slab, jnp.float32),
            pltpu.VMEM((ROWS, COLS), jnp.int32),
            pltpu.VMEM((DEPTH, TILES, ROWS + 2 * PAD, LANES), jnp.float32),
            pltpu.VMEM((TILES, ROWS + 2 * PAD, LANES), jnp.int32),
            pltpu.VMEM((ROWS, COLS), jnp.int32),
            *[column] * 8,
            *[pltpu.VMEM((ROWS, SENT * LANES), jnp.int32)] * 4,
            pltpu.VMEM((3, 8, LANES), jnp.int32),
            pltpu.VMEM((len(GROUPS) + 1, 8, LANES), jnp.int32),
            pltpu.VMEM((slots, 8, LANES), jnp.int32),
            pltpu.SemaphoreType.DMA((CHUNKS,)),
            pltpu.SemaphoreType.DMA((CHUNKS,)),
            pltpu.SemaphoreType.DMA((3, 2, CHUNKS)),
            pltpu.SemaphoreType.DMA((3, 2, CHUNKS)),
            pltpu.SemaphoreType.DMA((slots,)),
            pltpu.SemaphoreType.DMA((slots,)),
        ],
        compiler_params=pltpu.CompilerParams(
            collective_id=0, has_side_effects=True, vmem_limit_bytes=56 << 20
        ),
    )(scores)
    return pl.pallas_call(
        expand,
        out_shape=(
            jax.ShapeDtypeStruct(slab, jnp.int32),
            jax.ShapeDtypeStruct((3,), jnp.int32),
        ),
        grid=(ROWS // OUT_ROWS,),
        in_specs=[
            pl.BlockSpec((OUT_ROWS, COLS), lambda i: (i, 0)),
            pl.BlockSpec(memory_space=pltpu.SMEM),
        ],
        out_specs=(
            pl.BlockSpec((DEPTH, OUT_ROWS, COLS), lambda i: (0, i, 0)),
            pl.BlockSpec(memory_space=pltpu.SMEM),
        ),
    )(words, counts)


def solution(mesh):
    n = mesh.shape["gz"]
    return jax.shard_map(
        functools.partial(shards, n),
        mesh=mesh,
        in_specs=(P("gz", None, None),),
        out_specs=(P("gz", None, None), P()),
        check_vma=False,
    )
```

```python
import functools

import jax
import jax.numpy as jnp
from jax import lax
from jax.experimental import pallas as pl
from jax.experimental.pallas import tpu as pltpu
from jax.sharding import PartitionSpec as P

DEPTH = 4
ROWS = 512
COLS = 512
LANES = 128
TILES = 4
BLOCK = LANES // TILES
CHUNK = 32
CHUNKS = ROWS // CHUNK
STEP = 16
OUT_ROWS = 256
PAD = 8
GROUPS = (8, 16)
ROOT = float(1 << 40)
MANTISSA = 23
BITS = 27
SPARE = 32 - BITS
CARRIERS = 6
SENT = 2 * TILES - 1
MESH = pl.DeviceIdType.MESH


def cols(j):
    return slice(j * LANES, (j + 1) * LANES)


def gather(x, index):
    halves = [
        jnp.take_along_axis(x[r:r + 8], index, axis=1, mode="promise_in_bounds")
        for r in range(0, x.shape[0], 8)
    ]
    return jnp.concatenate(halves, axis=0)


def lane_of(height):
    return lax.broadcasted_iota(jnp.int32, (height, LANES), 1)


def by_block(tiles, source):
    block = lane_of(tiles[0].shape[0]) // BLOCK
    out = []
    for a in range(TILES):
        t = tiles[source(TILES - 1, a)]
        for p in range(TILES - 1):
            t = jnp.where(block == p, tiles[source(p, a)], t)
        out.append(t)
    return out


def interleave(tiles):
    lane = lane_of(8)
    sorted_ = [
        gather(t, (lane % BLOCK) * TILES + (lane // BLOCK + TILES - s) % TILES)
        for s, t in enumerate(tiles)
    ]
    mixed = by_block(sorted_, lambda p, j: (p - j) % TILES)
    return [pltpu.roll(t, LANES - BLOCK * j, 1) if j else t for j, t in enumerate(mixed)]


def natural(tiles):
    lane = lane_of(8)
    turned = [pltpu.roll(t, BLOCK * j, 1) if j else t for j, t in enumerate(tiles)]
    mixed = by_block(turned, lambda p, s: (p - s) % TILES)
    return [
        gather(t, BLOCK * ((lane % TILES + s) % TILES) + lane // TILES)
        for s, t in enumerate(mixed)
    ]


def column_sides(t):
    lane = lane_of(t[0].shape[0])
    zero = jnp.zeros(t[0].shape, t[0].dtype)
    before = [jnp.where(lane == 0, zero, pltpu.roll(t[j], 1, 1)) for j in (2, 3)]
    after = [jnp.where(lane == LANES - 1, zero, pltpu.roll(t[j], LANES - 1, 1)) for j in (0, 1)]
    return (*before, *after)


def column_window(t, sides, join):
    r2, r3, l0, l1 = sides
    m12 = join(t[1], t[2])
    m012, m123 = join(t[0], m12), join(m12, t[3])
    whole = join(m012, t[3])
    return [join(m012, join(r2, r3)), join(whole, r3), join(whole, l0), join(m123, join(l0, l1))]


def depth_max5(p):
    m34 = jnp.maximum(p[3], p[4])
    a = jnp.maximum(p[2], m34)
    a5 = jnp.maximum(a, p[5])
    return [
        jnp.maximum(jnp.maximum(p[0], p[1]), a),
        jnp.maximum(p[1], a5),
        jnp.maximum(a5, p[6]),
        jnp.maximum(jnp.maximum(m34, p[5]), jnp.maximum(p[6], p[7])),
    ]


def row_window(ref, at, row, join):
    parts = [ref[(*at, pl.ds(row + PAD + d, STEP), slice(None))] for d in (-2, -1, 0, 1, 2)]
    return join(join(join(parts[0], parts[1]), join(parts[3], parts[4])), parts[2])


def embed(s):
    low = (s & ((1 << MANTISSA) - 1)) | (1 << MANTISSA)
    exponent = jnp.right_shift(s, MANTISSA) & ((1 << (BITS - MANTISSA)) - 1)
    return low.astype(jnp.float32) * jnp.left_shift(jnp.ones_like(s), exponent).astype(jnp.float32)


def pack(tiles):
    *words, spare = tiles
    for i in range(CARRIERS):
        words[i] = words[i] | jnp.left_shift(jnp.right_shift(spare, SPARE * i), BITS)
    return words


def unpack(words):
    spare = None
    for i in range(CARRIERS):
        bits = jnp.left_shift(lax.shift_right_logical(words[i], BITS), SPARE * i)
        spare = bits if spare is None else spare | bits
    return [*words, spare]


def kernel(
    n, x_ref, out_ref, count_ref,
    x_buf, f_ref, l1_ref, l2_ref, gone_ref, t_ref, g_ref, st_ref,
    send_lo1, send_hi1, recv_lo1, recv_hi1, send_lo2, send_hi2, recv_lo2, recv_hi2,
    pack_lo, pack_hi, packed_lo, packed_hi, tally, part, parts,
    load_sem, store_sem, send_sems, recv_sems, part_send, part_recv,
):
    me = lax.axis_index("gz")
    right, left = lax.rem(me + 1, n), lax.rem(me + n - 1, n)
    has_left, has_right = me > 0, me < n - 1

    partners = []
    stride = 1
    for size in GROUPS:
        place = lax.rem(lax.div(me, stride), size)
        partners.append(
            [me + (lax.rem(place + o, size) - place) * stride for o in range(1, size)]
        )
        stride *= size

    def rows_of(c):
        return pl.ds(pl.multiple_of(c * CHUNK, CHUNK), CHUNK)

    def load(c):
        return pltpu.make_async_copy(
            x_ref.at[:, rows_of(c), :], x_buf.at[:, rows_of(c), :], load_sem.at[c]
        )

    def store(c):
        return pltpu.make_async_copy(
            st_ref.at[rows_of(c), :], out_ref.at[rows_of(c), :], store_sem.at[c]
        )

    def remote(src, dst, stage, side, c, device):
        return pltpu.make_async_remote_copy(
            src_ref=src, dst_ref=dst,
            send_sem=send_sems.at[stage, side, c], recv_sem=recv_sems.at[stage, side, c],
            device_id=(device,), device_id_type=MESH,
        )

    def planes(c):
        r = rows_of(c)
        return (
            remote(pack_lo.at[r, :], packed_hi.at[r, :], 0, 1, c, left),
            remote(pack_hi.at[r, :], packed_lo.at[r, :], 0, 0, c, right),
        )

    def roots1(c):
        r = rows_of(c)
        return (
            remote(send_lo1.at[r, :], recv_hi1.at[r, :], 1, 1, c, left),
            remote(send_hi1.at[r, :], recv_lo1.at[r, :], 1, 0, c, right),
        )

    def roots2(c):
        r = rows_of(c)
        return (
            remote(send_lo2.at[r, :], recv_hi2.at[r, :], 2, 1, c, left),
            remote(send_hi2.at[r, :], recv_lo2.at[r, :], 2, 0, c, right),
        )

    def sided(on_left, on_right):
        pl.when(has_left)(on_left)
        pl.when(has_right)(on_right)

    def start(pair):
        sided(pair[0].start, pair[1].start)

    def wait_recv(pair):
        sided(pair[1].wait_recv, pair[0].wait_recv)

    def wait_send(pair):
        sided(pair[0].wait_send, pair[1].wait_send)

    def loop(first, last, body):
        def step(i, carry):
            body(i)
            return carry
        lax.fori_loop(first, last, step, 0)

    def over_rows(c, body):
        loop(0, CHUNK // STEP, lambda i: body(pl.multiple_of(c * CHUNK + i * STEP, STEP)))

    loop(0, CHUNKS, lambda c: load(c).start())
    barrier = pltpu.get_barrier_semaphore()

    def greet(other):
        pl.semaphore_signal(barrier, inc=1, device_id=(other,), device_id_type=MESH)

    sided(lambda: greet(left), lambda: greet(right))
    greeted = [p for group in partners for p in group]
    for other in greeted:
        greet(other)

    def outside(*refs):
        def fill():
            def body(i):
                rows = pl.ds(pl.multiple_of(i * CHUNK, CHUNK), CHUNK)
                for ref in refs:
                    ref[rows, :] = jnp.zeros((CHUNK, ref.shape[1]), ref.dtype)
            loop(0, CHUNKS, body)
        return fill

    pl.when(jnp.logical_not(has_left))(outside(packed_lo, recv_lo1, recv_lo2))
    pl.when(jnp.logical_not(has_right))(outside(packed_hi, recv_hi1, recv_hi2))
    for j in range(TILES):
        for edge in (slice(0, PAD), slice(PAD + ROWS, 2 * PAD + ROWS)):
            for k in range(DEPTH):
                t_ref[k, j, edge, :] = jnp.zeros((PAD, LANES), jnp.float32)
            g_ref[j, edge, :] = jnp.zeros((PAD, LANES), jnp.int32)
    for k in range(3):
        tally[k] = jnp.zeros((8, LANES), jnp.int32)

    def prepare(c):
        load(c).wait()

        def body(row):
            own = []
            for k in range(DEPTH):
                tiles = [x_buf[k, pl.ds(row, STEP), cols(j)] for j in range(TILES)]
                own += interleave(tiles)
            for ref, tiles in ((pack_lo, own[:2 * TILES]), (pack_hi, own[2 * TILES:])):
                for i, word in enumerate(pack(tiles)):
                    ref[pl.ds(row, STEP), cols(i)] = word
            for i, t in enumerate(own):
                f_ref[2 + i // TILES, pl.ds(row, STEP), cols(i % TILES)] = embed(t)
        over_rows(c, body)

    def send_planes(c):
        prepare(c)
        start(planes(c))

    prepare(0)
    neighbours = has_left.astype(jnp.int32) + has_right.astype(jnp.int32)
    pl.semaphore_wait(barrier, neighbours + len(greeted))
    start(planes(0))
    loop(1, CHUNKS, send_planes)

    def rounds(first, second, arrive, leave):
        arrive(0)
        over_rows(0, lambda row: first(row)())

        def step(c):
            arrive(c)

            def body(row):
                first(row)()
                second(pl.multiple_of(row - CHUNK, STEP))
            over_rows(c, body)
            leave(c - 1)
        loop(1, CHUNKS, step)
        over_rows(CHUNKS - 1, second)
        leave(CHUNKS - 1)

    def add_count(k, flags):
        while len(flags) > 1:
            flags = [a + b for a, b in zip(flags[::2], flags[1::2])]
        tally[k] += flags[0][:8] + flags[0][8:]

    def sides_of(outs):
        return [column_sides([o[k] for o in outs]) for k in range(DEPTH)]

    def put(row, outs, sides):
        for k in range(DEPTH):
            tiles = column_window([o[k] for o in outs], sides[k], jnp.maximum)
            for j, t in enumerate(tiles):
                t_ref[k, j, pl.ds(row + PAD, STEP), :] = t

    def first1(row):
        outs, halos = [], []
        rows = pl.ds(row, STEP)
        low, high = (
            [embed(t) for t in unpack([ref[rows, cols(i)] for i in range(SENT)])]
            for ref in (packed_lo, packed_hi)
        )
        for j in range(TILES):
            at = (rows, cols(j))
            p = [
                low[j], low[TILES + j], *(f_ref[(k,) + at] for k in range(2, 6)),
                high[j], high[TILES + j],
            ]
            halos += [((k,) + at, p[k]) for k in (0, 1, 6, 7)]
            outs.append(depth_max5(p))
        sides = sides_of(outs)

        def finish():
            for at, value in halos:
                f_ref[at] = value
            put(row, outs, sides)
        return finish

    def second1(row):
        flags = []
        for j in range(TILES):
            at = (pl.ds(row, STEP), cols(j))
            roots = []
            for k in range(DEPTH):
                s = f_ref[(2 + k,) + at]
                root = row_window(t_ref, (k, j), row, jnp.maximum) == s
                l1_ref[(k,) + at] = jnp.where(root, ROOT, s)
                flags.append(jnp.where(root, 0, 1))
                roots.append(root)
            lo = jnp.zeros((STEP, LANES), jnp.float32)
            hi = lo
            for k in range(DEPTH):
                hi = jnp.where(roots[k], float(DEPTH - k), hi)
                lo = jnp.where(roots[DEPTH - 1 - k], float(DEPTH - k), lo)
            send_lo1[at] = lo.astype(jnp.bfloat16)
            send_hi1[at] = hi.astype(jnp.bfloat16)
        add_count(0, flags)

    rounds(first1, second1, lambda c: wait_recv(planes(c)), lambda c: start(roots1(c)))

    def first2(row):
        outs, marks = [], []
        for j in range(TILES):
            at = (pl.ds(row, STEP), cols(j))
            d_lo = recv_lo1[at].astype(jnp.float32)
            d_hi = recv_hi1[at].astype(jnp.float32)
            mine = [l1_ref[(k,) + at] for k in range(DEPTH)]
            outs.append(depth_max5([
                jnp.where(d_lo == 2.0, ROOT, f_ref[(0,) + at]),
                jnp.where(d_lo == 1.0, ROOT, f_ref[(1,) + at]),
                *mine,
                jnp.where(d_hi == 1.0, ROOT, f_ref[(6,) + at]),
                jnp.where(d_hi == 2.0, ROOT, f_ref[(7,) + at]),
            ]))
            mark = jnp.where(d_lo > 3.5, 1, jnp.where(d_lo > 0.5, 3, 0))
            mark |= jnp.where(d_hi > 3.5, 8, jnp.where(d_hi > 0.5, 12, 0))
            for value, bits in zip(mine, (3, 2, 4, 12)):
                mark |= jnp.where(value == ROOT, bits, 0)
            marks.append(mark)
        sides, mark_sides = sides_of(outs), column_sides(marks)

        def finish():
            put(row, outs, sides)
            for j, t in enumerate(column_window(marks, mark_sides, jnp.bitwise_or)):
                g_ref[j, pl.ds(row + PAD, STEP), :] = t
        return finish

    def second2(row):
        flags = []
        for j in range(TILES):
            at = (pl.ds(row, STEP), cols(j))
            roots = []
            for k in range(DEPTH):
                l = l1_ref[(k,) + at]
                top = row_window(t_ref, (k, j), row, jnp.maximum)
                root, near = top == l, top >= ROOT
                value = jnp.where(root, ROOT, jnp.where(near, 0.0, l))
                l2_ref[(k,) + at] = value
                flags.append(jnp.where(root | near, 0, 1))
                roots.append(root)
            gone_ref[at] = row_window(g_ref, (j,), row, jnp.bitwise_or)
            lo = jnp.where(roots[0], 1.0, jnp.where(roots[1], 2.0, 0.0))
            hi = jnp.where(roots[3], 1.0, jnp.where(roots[2], 2.0, 0.0))
            send_lo2[at] = lo.astype(jnp.bfloat16)
            send_hi2[at] = hi.astype(jnp.bfloat16)
        add_count(1, flags)

    rounds(first2, second2, lambda c: wait_recv(roots1(c)), lambda c: start(roots2(c)))

    def first3(row):
        outs = []
        for j in range(TILES):
            at = (pl.ds(row, STEP), cols(j))
            d_lo = recv_lo2[at].astype(jnp.float32)
            d_hi = recv_hi2[at].astype(jnp.float32)
            gone = gone_ref[at]

            def halo(k, bit, is_root):
                left_over = jnp.where((gone & bit) == 0, f_ref[(k,) + at], 0.0)
                return jnp.where(is_root, ROOT, left_over)

            outs.append(depth_max5([
                halo(0, 1, d_lo == 2.0), halo(1, 2, d_lo == 1.0),
                *(l2_ref[(k,) + at] for k in range(DEPTH)),
                halo(6, 4, d_hi == 1.0), halo(7, 8, d_hi == 2.0),
            ]))
        sides = sides_of(outs)
        return lambda: put(row, outs, sides)

    def second3(row):
        flags = []
        for j in range(TILES):
            at = (pl.ds(row, STEP), cols(j))
            word = None
            for k in range(DEPTH):
                top = row_window(t_ref, (k, j), row, jnp.maximum)
                root, near = top == l2_ref[(k,) + at], top >= ROOT
                state = jnp.where(root, 1 << 2 * k, jnp.where(near, 2 << 2 * k, 0))
                word = state if word is None else word | state
                flags.append(jnp.where(root | near, 0, 1))
            st_ref[at] = word
        add_count(2, flags)

    rounds(first3, second3, lambda c: wait_recv(roots2(c)), lambda c: store(c).start())

    for k in range(3):
        part[0, k:k + 1, :] = jnp.sum(tally[k], axis=0, keepdims=True)
    part[0, 3:8, :] = jnp.zeros((5, LANES), jnp.int32)
    slot = 0
    for stage, group in enumerate(partners):
        copies = [
            pltpu.make_async_remote_copy(
                src_ref=part.at[stage], dst_ref=parts.at[slot + o],
                send_sem=part_send.at[slot + o], recv_sem=part_recv.at[slot + o],
                device_id=(other,), device_id_type=MESH,
            )
            for o, other in enumerate(group)
        ]
        for copy in copies:
            copy.start()
        total = part[stage]
        for o, copy in enumerate(copies):
            copy.wait_recv()
            total = total + parts[slot + o]
        part[stage + 1] = total
        for copy in copies:
            copy.wait_send()
        slot += len(group)
    for k in range(3):
        count_ref[k] = jnp.sum(part[len(GROUPS), k:k + 1, :])

    def drain(c):
        wait_send(planes(c))
        wait_send(roots1(c))
        wait_send(roots2(c))
        store(c).wait()

    loop(0, CHUNKS, drain)


def expand(word_ref, count_ref, out_ref, count_out_ref):
    for j, words in enumerate(natural([word_ref[:, cols(j)] for j in range(TILES)])):
        for k in range(DEPTH):
            out_ref[k, :, cols(j)] = jnp.right_shift(words, 2 * k) & 3
    for k in range(3):
        count_out_ref[k] = count_ref[k]


def shards(n, scores):
    slab = (DEPTH, ROWS, COLS)
    column = pltpu.VMEM((ROWS, COLS), jnp.bfloat16)
    slots = sum(GROUPS) - len(GROUPS)
    words, counts = pl.pallas_call(
        functools.partial(kernel, n),
        out_shape=(
            jax.ShapeDtypeStruct((ROWS, COLS), jnp.int32),
            jax.ShapeDtypeStruct((3,), jnp.int32),
        ),
        in_specs=[pl.BlockSpec(memory_space=pl.ANY)],
        out_specs=(
            pl.BlockSpec(memory_space=pl.ANY),
            pl.BlockSpec(memory_space=pltpu.SMEM),
        ),
        scratch_shapes=[
            pltpu.VMEM(slab, jnp.int32),
            pltpu.VMEM((2 * DEPTH, ROWS, COLS), jnp.float32),
            pltpu.VMEM(slab, jnp.float32),
            pltpu.VMEM(slab, jnp.float32),
            pltpu.VMEM((ROWS, COLS), jnp.int32),
            pltpu.VMEM((DEPTH, TILES, ROWS + 2 * PAD, LANES), jnp.float32),
            pltpu.VMEM((TILES, ROWS + 2 * PAD, LANES), jnp.int32),
            pltpu.VMEM((ROWS, COLS), jnp.int32),
            *[column] * 8,
            *[pltpu.VMEM((ROWS, SENT * LANES), jnp.int32)] * 4,
            pltpu.VMEM((3, 8, LANES), jnp.int32),
            pltpu.VMEM((len(GROUPS) + 1, 8, LANES), jnp.int32),
            pltpu.VMEM((slots, 8, LANES), jnp.int32),
            pltpu.SemaphoreType.DMA((CHUNKS,)),
            pltpu.SemaphoreType.DMA((CHUNKS,)),
            pltpu.SemaphoreType.DMA((3, 2, CHUNKS)),
            pltpu.SemaphoreType.DMA((3, 2, CHUNKS)),
            pltpu.SemaphoreType.DMA((slots,)),
            pltpu.SemaphoreType.DMA((slots,)),
        ],
        compiler_params=pltpu.CompilerParams(
            collective_id=0, has_side_effects=True, vmem_limit_bytes=56 << 20
        ),
    )(scores)
    return pl.pallas_call(
        expand,
        out_shape=(
            jax.ShapeDtypeStruct(slab, jnp.int32),
            jax.ShapeDtypeStruct((3,), jnp.int32),
        ),
        grid=(ROWS // OUT_ROWS,),
        in_specs=[
            pl.BlockSpec((OUT_ROWS, COLS), lambda i: (i, 0)),
            pl.BlockSpec(memory_space=pltpu.SMEM),
        ],
        out_specs=(
            pl.BlockSpec((DEPTH, OUT_ROWS, COLS), lambda i: (0, i, 0)),
            pl.BlockSpec(memory_space=pltpu.SMEM),
        ),
    )(words, counts)


def solution(mesh):
    n = mesh.shape["gz"]
    return jax.shard_map(
        functools.partial(shards, n),
        mesh=mesh,
        in_specs=(P("gz", None, None),),
        out_specs=(P("gz", None, None), P()),
        check_vma=False,
    )
```

```python
import functools

import jax
import jax.numpy as jnp
from jax import lax
from jax.experimental import pallas as pl
from jax.experimental.pallas import tpu as pltpu
from jax.sharding import PartitionSpec as P

DEPTH = 4
ROWS = 512
COLS = 512
LANES = 128
TILES = 4
BLOCK = LANES // TILES
CHUNK = 32
CHUNKS = ROWS // CHUNK
STEP = 16
OUT_ROWS = 256
PAD = 8
GROUPS = (8, 16)
ROOT = float(1 << 40)
MANTISSA = 23
BITS = 27
SPARE = 32 - BITS
CARRIERS = 6
SENT = 2 * TILES - 1
MESH = pl.DeviceIdType.MESH


def cols(j):
    return slice(j * LANES, (j + 1) * LANES)


def gather(x, index):
    halves = [
        jnp.take_along_axis(x[r:r + 8], index, axis=1, mode="promise_in_bounds")
        for r in range(0, x.shape[0], 8)
    ]
    return jnp.concatenate(halves, axis=0)


def lane_of(height):
    return lax.broadcasted_iota(jnp.int32, (height, LANES), 1)


def by_block(tiles, source):
    block = lane_of(tiles[0].shape[0]) // BLOCK
    out = []
    for a in range(TILES):
        t = tiles[source(TILES - 1, a)]
        for p in range(TILES - 1):
            t = jnp.where(block == p, tiles[source(p, a)], t)
        out.append(t)
    return out


def interleave(tiles):
    lane = lane_of(8)
    sorted_ = [
        gather(t, (lane % BLOCK) * TILES + (lane // BLOCK + TILES - s) % TILES)
        for s, t in enumerate(tiles)
    ]
    mixed = by_block(sorted_, lambda p, j: (p - j) % TILES)
    return [pltpu.roll(t, LANES - BLOCK * j, 1) if j else t for j, t in enumerate(mixed)]


def natural(tiles):
    lane = lane_of(8)
    turned = [pltpu.roll(t, BLOCK * j, 1) if j else t for j, t in enumerate(tiles)]
    mixed = by_block(turned, lambda p, s: (p - s) % TILES)
    return [
        gather(t, BLOCK * ((lane % TILES + s) % TILES) + lane // TILES)
        for s, t in enumerate(mixed)
    ]


def column_sides(t):
    lane = lane_of(t[0].shape[0])
    zero = jnp.zeros(t[0].shape, t[0].dtype)
    before = [jnp.where(lane == 0, zero, pltpu.roll(t[j], 1, 1)) for j in (2, 3)]
    after = [jnp.where(lane == LANES - 1, zero, pltpu.roll(t[j], LANES - 1, 1)) for j in (0, 1)]
    return (*before, *after)


def column_window(t, sides, join):
    r2, r3, l0, l1 = sides
    m12 = join(t[1], t[2])
    m012, m123 = join(t[0], m12), join(m12, t[3])
    whole = join(m012, t[3])
    return [join(m012, join(r2, r3)), join(whole, r3), join(whole, l0), join(m123, join(l0, l1))]


def depth_max5(p):
    m34 = jnp.maximum(p[3], p[4])
    a = jnp.maximum(p[2], m34)
    a5 = jnp.maximum(a, p[5])
    return [
        jnp.maximum(jnp.maximum(p[0], p[1]), a),
        jnp.maximum(p[1], a5),
        jnp.maximum(a5, p[6]),
        jnp.maximum(jnp.maximum(m34, p[5]), jnp.maximum(p[6], p[7])),
    ]


def row_window(ref, at, row, join):
    parts = [ref[(*at, pl.ds(row + PAD + d, STEP), slice(None))] for d in (-2, -1, 0, 1, 2)]
    return join(join(join(parts[0], parts[1]), join(parts[3], parts[4])), parts[2])


def embed(s):
    low = (s & ((1 << MANTISSA) - 1)) | (1 << MANTISSA)
    exponent = jnp.right_shift(s, MANTISSA) & ((1 << (BITS - MANTISSA)) - 1)
    return low.astype(jnp.float32) * jnp.left_shift(jnp.ones_like(s), exponent).astype(jnp.float32)


def pack(tiles):
    *words, spare = tiles
    for i in range(CARRIERS):
        words[i] = words[i] | jnp.left_shift(jnp.right_shift(spare, SPARE * i), BITS)
    return words


def unpack(words):
    spare = None
    for i in range(CARRIERS):
        bits = jnp.left_shift(lax.shift_right_logical(words[i], BITS), SPARE * i)
        spare = bits if spare is None else spare | bits
    return [*words, spare]


def kernel(
    n, x_ref, out_ref, count_ref,
    x_buf, f_ref, l1_ref, l2_ref, gone_ref, t_ref, g_ref, st_ref,
    send_lo1, send_hi1, recv_lo1, recv_hi1, send_lo2, send_hi2, recv_lo2, recv_hi2,
    pack_lo, pack_hi, packed_lo, packed_hi, tally, part, parts,
    load_sem, store_sem, send_sems, recv_sems, part_send, part_recv,
):
    me = lax.axis_index("gz")
    right, left = lax.rem(me + 1, n), lax.rem(me + n - 1, n)
    has_left, has_right = me > 0, me < n - 1

    partners = []
    stride = 1
    for size in GROUPS:
        place = lax.rem(lax.div(me, stride), size)
        partners.append(
            [me + (lax.rem(place + o, size) - place) * stride for o in range(1, size)]
        )
        stride *= size

    def rows_of(c):
        return pl.ds(pl.multiple_of(c * CHUNK, CHUNK), CHUNK)

    def load(c):
        return pltpu.make_async_copy(
            x_ref.at[:, rows_of(c), :], x_buf.at[:, rows_of(c), :], load_sem.at[c]
        )

    def store(c):
        return pltpu.make_async_copy(
            st_ref.at[rows_of(c), :], out_ref.at[rows_of(c), :], store_sem.at[c]
        )

    def remote(src, dst, stage, side, c, device):
        return pltpu.make_async_remote_copy(
            src_ref=src, dst_ref=dst,
            send_sem=send_sems.at[stage, side, c], recv_sem=recv_sems.at[stage, side, c],
            device_id=(device,), device_id_type=MESH,
        )

    def planes(c):
        r = rows_of(c)
        return (
            remote(pack_lo.at[r, :], packed_hi.at[r, :], 0, 1, c, left),
            remote(pack_hi.at[r, :], packed_lo.at[r, :], 0, 0, c, right),
        )

    def roots1(c):
        r = rows_of(c)
        return (
            remote(send_lo1.at[r, :], recv_hi1.at[r, :], 1, 1, c, left),
            remote(send_hi1.at[r, :], recv_lo1.at[r, :], 1, 0, c, right),
        )

    def roots2(c):
        r = rows_of(c)
        return (
            remote(send_lo2.at[r, :], recv_hi2.at[r, :], 2, 1, c, left),
            remote(send_hi2.at[r, :], recv_lo2.at[r, :], 2, 0, c, right),
        )

    def sided(on_left, on_right):
        pl.when(has_left)(on_left)
        pl.when(has_right)(on_right)

    def start(pair):
        sided(pair[0].start, pair[1].start)

    def wait_recv(pair):
        sided(pair[1].wait_recv, pair[0].wait_recv)

    def wait_send(pair):
        sided(pair[0].wait_send, pair[1].wait_send)

    def loop(first, last, body):
        def step(i, carry):
            body(i)
            return carry
        lax.fori_loop(first, last, step, 0)

    def over_rows(c, body):
        loop(0, CHUNK // STEP, lambda i: body(pl.multiple_of(c * CHUNK + i * STEP, STEP)))

    barrier = pltpu.get_barrier_semaphore()

    def greet(other):
        pl.semaphore_signal(barrier, inc=1, device_id=(other,), device_id_type=MESH)

    sided(lambda: greet(left), lambda: greet(right))
    greeted = [p for group in partners for p in group]
    for other in greeted:
        greet(other)
    loop(0, CHUNKS, lambda c: load(c).start())

    def outside(*refs):
        def fill():
            def body(i):
                rows = pl.ds(pl.multiple_of(i * CHUNK, CHUNK), CHUNK)
                for ref in refs:
                    ref[rows, :] = jnp.zeros((CHUNK, ref.shape[1]), ref.dtype)
            loop(0, CHUNKS, body)
        return fill

    pl.when(jnp.logical_not(has_left))(outside(packed_lo, recv_lo1, recv_lo2))
    pl.when(jnp.logical_not(has_right))(outside(packed_hi, recv_hi1, recv_hi2))
    for j in range(TILES):
        for edge in (slice(0, PAD), slice(PAD + ROWS, 2 * PAD + ROWS)):
            for k in range(DEPTH):
                t_ref[k, j, edge, :] = jnp.zeros((PAD, LANES), jnp.float32)
            g_ref[j, edge, :] = jnp.zeros((PAD, LANES), jnp.int32)
    for k in range(3):
        tally[k] = jnp.zeros((8, LANES), jnp.int32)

    def prepare(c):
        load(c).wait()

        def body(row):
            own = []
            for k in range(DEPTH):
                tiles = [x_buf[k, pl.ds(row, STEP), cols(j)] for j in range(TILES)]
                own += interleave(tiles)
            for ref, tiles in ((pack_lo, own[:2 * TILES]), (pack_hi, own[2 * TILES:])):
                for i, word in enumerate(pack(tiles)):
                    ref[pl.ds(row, STEP), cols(i)] = word
            for i, t in enumerate(own):
                f_ref[2 + i // TILES, pl.ds(row, STEP), cols(i % TILES)] = embed(t)
        over_rows(c, body)

    def send_planes(c):
        prepare(c)
        start(planes(c))

    prepare(0)
    neighbours = has_left.astype(jnp.int32) + has_right.astype(jnp.int32)
    pl.semaphore_wait(barrier, neighbours + len(greeted))
    start(planes(0))
    loop(1, CHUNKS, send_planes)

    def rounds(first, second, arrive, leave):
        arrive(0)
        over_rows(0, lambda row: first(row)())

        def step(c):
            arrive(c)

            def body(row):
                first(row)()
                second(pl.multiple_of(row - CHUNK, STEP))
            over_rows(c, body)
            leave(c - 1)
        loop(1, CHUNKS, step)
        over_rows(CHUNKS - 1, second)
        leave(CHUNKS - 1)

    def add_count(k, flags):
        while len(flags) > 1:
            flags = [a + b for a, b in zip(flags[::2], flags[1::2])]
        tally[k] += flags[0][:8] + flags[0][8:]

    def sides_of(outs):
        return [column_sides([o[k] for o in outs]) for k in range(DEPTH)]

    def put(row, outs, sides):
        for k in range(DEPTH):
            tiles = column_window([o[k] for o in outs], sides[k], jnp.maximum)
            for j, t in enumerate(tiles):
                t_ref[k, j, pl.ds(row + PAD, STEP), :] = t

    def first1(row):
        outs, halos = [], []
        rows = pl.ds(row, STEP)
        low, high = (
            [embed(t) for t in unpack([ref[rows, cols(i)] for i in range(SENT)])]
            for ref in (packed_lo, packed_hi)
        )
        for j in range(TILES):
            at = (rows, cols(j))
            p = [
                low[j], low[TILES + j], *(f_ref[(k,) + at] for k in range(2, 6)),
                high[j], high[TILES + j],
            ]
            halos += [((k,) + at, p[k]) for k in (0, 1, 6, 7)]
            outs.append(depth_max5(p))
        sides = sides_of(outs)

        def finish():
            for at, value in halos:
                f_ref[at] = value
            put(row, outs, sides)
        return finish

    def second1(row):
        flags = []
        for j in range(TILES):
            at = (pl.ds(row, STEP), cols(j))
            roots = []
            for k in range(DEPTH):
                s = f_ref[(2 + k,) + at]
                root = row_window(t_ref, (k, j), row, jnp.maximum) == s
                l1_ref[(k,) + at] = jnp.where(root, ROOT, s)
                flags.append(jnp.where(root, 0, 1))
                roots.append(root)
            lo = jnp.zeros((STEP, LANES), jnp.float32)
            hi = lo
            for k in range(DEPTH):
                hi = jnp.where(roots[k], float(DEPTH - k), hi)
                lo = jnp.where(roots[DEPTH - 1 - k], float(DEPTH - k), lo)
            send_lo1[at] = lo.astype(jnp.bfloat16)
            send_hi1[at] = hi.astype(jnp.bfloat16)
        add_count(0, flags)

    rounds(first1, second1, lambda c: wait_recv(planes(c)), lambda c: start(roots1(c)))

    def first2(row):
        outs, marks = [], []
        for j in range(TILES):
            at = (pl.ds(row, STEP), cols(j))
            d_lo = recv_lo1[at].astype(jnp.float32)
            d_hi = recv_hi1[at].astype(jnp.float32)
            mine = [l1_ref[(k,) + at] for k in range(DEPTH)]
            outs.append(depth_max5([
                jnp.where(d_lo == 2.0, ROOT, f_ref[(0,) + at]),
                jnp.where(d_lo == 1.0, ROOT, f_ref[(1,) + at]),
                *mine,
                jnp.where(d_hi == 1.0, ROOT, f_ref[(6,) + at]),
                jnp.where(d_hi == 2.0, ROOT, f_ref[(7,) + at]),
            ]))
            mark = jnp.where(d_lo > 3.5, 1, jnp.where(d_lo > 0.5, 3, 0))
            mark |= jnp.where(d_hi > 3.5, 8, jnp.where(d_hi > 0.5, 12, 0))
            for value, bits in zip(mine, (3, 2, 4, 12)):
                mark |= jnp.where(value == ROOT, bits, 0)
            marks.append(mark)
        sides, mark_sides = sides_of(outs), column_sides(marks)

        def finish():
            put(row, outs, sides)
            for j, t in enumerate(column_window(marks, mark_sides, jnp.bitwise_or)):
                g_ref[j, pl.ds(row + PAD, STEP), :] = t
        return finish

    def second2(row):
        flags = []
        for j in range(TILES):
            at = (pl.ds(row, STEP), cols(j))
            roots = []
            for k in range(DEPTH):
                l = l1_ref[(k,) + at]
                top = row_window(t_ref, (k, j), row, jnp.maximum)
                root, near = top == l, top >= ROOT
                value = jnp.where(root, ROOT, jnp.where(near, 0.0, l))
                l2_ref[(k,) + at] = value
                flags.append(jnp.where(root | near, 0, 1))
                roots.append(root)
            gone_ref[at] = row_window(g_ref, (j,), row, jnp.bitwise_or)
            lo = jnp.where(roots[0], 1.0, jnp.where(roots[1], 2.0, 0.0))
            hi = jnp.where(roots[3], 1.0, jnp.where(roots[2], 2.0, 0.0))
            send_lo2[at] = lo.astype(jnp.bfloat16)
            send_hi2[at] = hi.astype(jnp.bfloat16)
        add_count(1, flags)

    rounds(first2, second2, lambda c: wait_recv(roots1(c)), lambda c: start(roots2(c)))

    def first3(row):
        outs = []
        for j in range(TILES):
            at = (pl.ds(row, STEP), cols(j))
            d_lo = recv_lo2[at].astype(jnp.float32)
            d_hi = recv_hi2[at].astype(jnp.float32)
            gone = gone_ref[at]

            def halo(k, bit, is_root):
                left_over = jnp.where((gone & bit) == 0, f_ref[(k,) + at], 0.0)
                return jnp.where(is_root, ROOT, left_over)

            outs.append(depth_max5([
                halo(0, 1, d_lo == 2.0), halo(1, 2, d_lo == 1.0),
                *(l2_ref[(k,) + at] for k in range(DEPTH)),
                halo(6, 4, d_hi == 1.0), halo(7, 8, d_hi == 2.0),
            ]))
        sides = sides_of(outs)
        return lambda: put(row, outs, sides)

    def second3(row):
        flags = []
        for j in range(TILES):
            at = (pl.ds(row, STEP), cols(j))
            word = None
            for k in range(DEPTH):
                top = row_window(t_ref, (k, j), row, jnp.maximum)
                root, near = top == l2_ref[(k,) + at], top >= ROOT
                state = jnp.where(root, 1 << 2 * k, jnp.where(near, 2 << 2 * k, 0))
                word = state if word is None else word | state
                flags.append(jnp.where(root | near, 0, 1))
            st_ref[at] = word
        add_count(2, flags)

    rounds(first3, second3, lambda c: wait_recv(roots2(c)), lambda c: store(c).start())

    for k in range(3):
        part[0, k:k + 1, :] = jnp.sum(tally[k], axis=0, keepdims=True)
    part[0, 3:8, :] = jnp.zeros((5, LANES), jnp.int32)
    slot = 0
    for stage, group in enumerate(partners):
        copies = [
            pltpu.make_async_remote_copy(
                src_ref=part.at[stage], dst_ref=parts.at[slot + o],
                send_sem=part_send.at[slot + o], recv_sem=part_recv.at[slot + o],
                device_id=(other,), device_id_type=MESH,
            )
            for o, other in enumerate(group)
        ]
        for copy in copies:
            copy.start()
        total = part[stage]
        for o, copy in enumerate(copies):
            copy.wait_recv()
            total = total + parts[slot + o]
        part[stage + 1] = total
        for copy in copies:
            copy.wait_send()
        slot += len(group)
    for k in range(3):
        count_ref[k] = jnp.sum(part[len(GROUPS), k:k + 1, :])

    def drain(c):
        wait_send(planes(c))
        wait_send(roots1(c))
        wait_send(roots2(c))
        store(c).wait()

    loop(0, CHUNKS, drain)


def expand(word_ref, count_ref, out_ref, count_out_ref):
    for j, words in enumerate(natural([word_ref[:, cols(j)] for j in range(TILES)])):
        for k in range(DEPTH):
            out_ref[k, :, cols(j)] = jnp.right_shift(words, 2 * k) & 3
    for k in range(3):
        count_out_ref[k] = count_ref[k]


def shards(n, scores):
    slab = (DEPTH, ROWS, COLS)
    column = pltpu.VMEM((ROWS, COLS), jnp.bfloat16)
    slots = sum(GROUPS) - len(GROUPS)
    words, counts = pl.pallas_call(
        functools.partial(kernel, n),
        out_shape=(
            jax.ShapeDtypeStruct((ROWS, COLS), jnp.int32),
            jax.ShapeDtypeStruct((3,), jnp.int32),
        ),
        in_specs=[pl.BlockSpec(memory_space=pl.ANY)],
        out_specs=(
            pl.BlockSpec(memory_space=pl.ANY),
            pl.BlockSpec(memory_space=pltpu.SMEM),
        ),
        scratch_shapes=[
            pltpu.VMEM(slab, jnp.int32),
            pltpu.VMEM((2 * DEPTH, ROWS, COLS), jnp.float32),
            pltpu.VMEM(slab, jnp.float32),
            pltpu.VMEM(slab, jnp.float32),
            pltpu.VMEM((ROWS, COLS), jnp.int32),
            pltpu.VMEM((DEPTH, TILES, ROWS + 2 * PAD, LANES), jnp.float32),
            pltpu.VMEM((TILES, ROWS + 2 * PAD, LANES), jnp.int32),
            pltpu.VMEM((ROWS, COLS), jnp.int32),
            *[column] * 8,
            *[pltpu.VMEM((ROWS, SENT * LANES), jnp.int32)] * 4,
            pltpu.VMEM((3, 8, LANES), jnp.int32),
            pltpu.VMEM((len(GROUPS) + 1, 8, LANES), jnp.int32),
            pltpu.VMEM((slots, 8, LANES), jnp.int32),
            pltpu.SemaphoreType.DMA((CHUNKS,)),
            pltpu.SemaphoreType.DMA((CHUNKS,)),
            pltpu.SemaphoreType.DMA((3, 2, CHUNKS)),
            pltpu.SemaphoreType.DMA((3, 2, CHUNKS)),
            pltpu.SemaphoreType.DMA((slots,)),
            pltpu.SemaphoreType.DMA((slots,)),
        ],
        compiler_params=pltpu.CompilerParams(
            collective_id=0, has_side_effects=True, vmem_limit_bytes=56 << 20
        ),
    )(scores)
    return pl.pallas_call(
        expand,
        out_shape=(
            jax.ShapeDtypeStruct(slab, jnp.int32),
            jax.ShapeDtypeStruct((3,), jnp.int32),
        ),
        grid=(ROWS // OUT_ROWS,),
        in_specs=[
            pl.BlockSpec((OUT_ROWS, COLS), lambda i: (i, 0)),
            pl.BlockSpec(memory_space=pltpu.SMEM),
        ],
        out_specs=(
            pl.BlockSpec((DEPTH, OUT_ROWS, COLS), lambda i: (0, i, 0)),
            pl.BlockSpec(memory_space=pltpu.SMEM),
        ),
    )(words, counts)


def solution(mesh):
    n = mesh.shape["gz"]
    return jax.shard_map(
        functools.partial(shards, n),
        mesh=mesh,
        in_specs=(P("gz", None, None),),
        out_specs=(P("gz", None, None), P()),
        check_vma=False,
    )
```
